128 devices in a mesh: row: 16 (over y, x_lo, core), col: 8 (over x_hi, z).
Axes of the slice: x: 4 (x_hi: 2, x_lo: 2; x = x_hi * 2 + x_lo), y: 4, z: 4, core: 2. Of those that a mesh axis runs over, the one named last changes fastest.
Arguments:
- adjacency: int32 [10240, 320], P('row', 'col'), may hold values from -2147483648 to 2147483647, as said below
- relabel: int32 [10240], P(('row', 'col')), may hold values from 0 to 10239, each once
Outputs:
- clustering: float32 [10240], P(('row', 'col'))
- transitivity: float32 [], replicated
The draws below stay inside these ranges and needn't reach their ends.
Inputs may be any that keep to these rules, and one draw needn't show every extreme that they name: The unpacked adjacency is symmetric with a zero diagonal.
All inputs are finite; a program needn't handle non-finite values.
Results may differ from the reference program's by a relative error of at most 0.0003.
Values sent between devices are 32-bit elements.
A program may use at most 128 MiB of HBM per device.

```python
import jax
import jax.numpy as jnp
from jax import lax

NV = 10240
N_ROW = 16


def draw_adjacency(key, part):
    first, second = jax.random.split(jax.random.fold_in(key, 23), 2)
    activity = jax.random.randint(first, (NV,), 1, 5)
    thresh = 1000 * activity[:, None] * activity[None, :]
    coins = jax.random.randint(second, (NV, NV), 0, 65536)
    keep = coins < thresh
    index = jnp.arange(NV)
    upper = keep & (index[None, :] > index[:, None])
    links = (upper | upper.T).astype(jnp.int32)
    bits = links.reshape(NV, NV // 32, 32)
    shifts = jnp.arange(32, dtype=jnp.int32)
    words = jnp.sum(lax.shift_left(bits, shifts[None, None, :]), axis=2)
    return words.astype(jnp.int32)


def setup_inputs(seed: int = 0) -> dict:
    key_list = jax.random.split(jax.random.key(seed), 3)
    return {
        "adjacency": draw_adjacency(jax.random.fold_in(key_list[2], 71), 0),
        "relabel": jax.random.permutation(key_list[1], NV).astype(jnp.int32),
    }


def unpack(words):
    shifts = jnp.arange(32, dtype=jnp.int32)
    bits = lax.shift_right_logical(words[:, :, None], shifts[None, None, :]) & 1
    return bits.reshape(words.shape[0], words.shape[1] * 32).astype(jnp.bfloat16)


def reference(adjacency, relabel):
    links = unpack(adjacency)
    block_rows = NV // N_ROW
    starts = jnp.arange(N_ROW, dtype=jnp.int32) * block_rows

    def one_block(offset):
        rows = lax.dynamic_slice_in_dim(links, offset.astype(jnp.int32), block_rows, 0)
        paths = jnp.dot(rows, links, preferred_element_type=jnp.float32)
        wide = rows.astype(jnp.float32)
        return jnp.sum(wide * paths, axis=1), jnp.sum(wide, axis=1)

    closed, degree = lax.map(one_block, starts)
    closed = closed.reshape(NV)
    degree = degree.reshape(NV)
    wedges = jnp.maximum(degree * (degree - 1.0), 1.0)
    ratio = closed / wedges
    clustering = jnp.take(ratio, relabel, axis=0)
    transitivity = jnp.sum(closed) / jnp.sum(wedges)
    return clustering, transitivity
```

```python
import jax
import jax.numpy as jnp
from jax import lax
from jax.experimental import pallas as pl
from jax.experimental.pallas import tpu as pltpu
from jax.sharding import PartitionSpec as P

G0 = (0, 4, 1, 5, 6, 2, 7, 3)
G1 = (0, 7, 6, 1, 3, 4, 5, 2)
E0 = (0, 2, 5, 7, 1, 3, 4, 6)
E1 = (0, 3, 7, 4, 5, 6, 2, 1)
F8 = jnp.float8_e4m3fn
I32 = jnp.int32
WORDS, ROWS, WIDE = 40, 640, 1280
TILE = 256


def look_up(table, d):
    return sum(jnp.where(d == i, I32(v), I32(0)) for i, v in enumerate(table) if v)


def xor3(a, b):
    out = I32(0)
    for bit in (1, 2, 4):
        p, q = (a // bit) % 2, (b // bit) % 2
        out = out + bit * (p + q - 2 * p * q)
    return out


def bits_of(row, mask, kind):
    wide = jnp.broadcast_to(row, (32, row.shape[1]))
    return jnp.where((wide & mask) != 0, 1.0, 0.0).astype(kind)


def kernel(
    adj, rel, out,
    own, rhs, lhs, w_rhs, w_lhs, acc, part_row, part_col, red_row, red_col, mine, every,
    send, rhs_sem, lhs_sem, relay_sem, row_sem, col_sem, all_send, all_sem,
):
    row, col = lax.axis_index("row"), lax.axis_index("col")
    R, C, h = row // 2, col, row % 2
    d = xor3(R, C)
    diag, off = d == 0, d != 0

    barrier = pltpu.get_barrier_semaphore()

    def hello(r, c):
        pl.semaphore_signal(barrier, inc=1, device_id={"row": r, "col": c})

    @pl.loop(1, 8)
    def _(i):
        for g in range(2):
            hello(2 * R + g, (C + i) % 8)
            hello(2 * ((R + i) % 8) + g, C)

    hello(2 * R + 1 - h, C)
    own[...] = adj[...].T

    @pl.when(diag)
    def _():
        lhs[2, h] = own[...]

    pl.semaphore_wait(barrier, 29)

    def copy(src, dst, ssem, rsem, r, c):
        return pltpu.make_async_remote_copy(
            src_ref=src, dst_ref=dst, send_sem=ssem, recv_sem=rsem,
            device_id={"row": r, "col": c},
        )

    def relay(s):
        return copy(lhs.at[s, h], lhs.at[s, h], send.at[7 + s], relay_sem.at[s], 2 * R + 1 - h, C)

    offers = []
    for j, (g, e) in enumerate(((G0, E0), (G1, E1))):
        to = xor3(R, xor3(d, look_up(g, d)))
        offers.append(copy(own, rhs.at[1 - j], send.at[2 * j], rhs_sem.at[1 - j], row, to))
        to = xor3(C, look_up(e, d))
        offers.append(
            copy(own, lhs.at[j, h], send.at[2 * j + 1], lhs_sem.at[j], 2 * to + h, C)
        )

    spread = [
        copy(own, lhs.at[2, h], send.at[i - 1], lhs_sem.at[2], 2 * ((R + i) % 8) + h, C)
        for i in range(1, 8)
    ]

    @pl.when(off)
    def _():
        for c in offers:
            c.start()

    @pl.when(diag)
    def _():
        for c in spread:
            c.start()
        relay(2).start()

    mask = jnp.left_shift(I32(1), lax.broadcasted_iota(I32, (32, ROWS), 0))

    def unpack_rhs(src):
        @pl.loop(0, 5)
        def _(i):
            base = pl.multiple_of(i * 8, 8)
            for w in range(8):
                at = pl.multiple_of(i * 256 + w * 32, 32)
                w_rhs[pl.ds(at, 32), :] = bits_of(src[pl.ds(base + w, 1), :], mask, F8)

    def product(s, first):
        @pl.loop(0, WIDE // TILE)
        def _(i):
            base = pl.multiple_of(i * (TILE // 32), TILE // 32)
            for g in range(2):
                for w in range(TILE // 32):
                    w_lhs[w * 32 : (w + 1) * 32, g * ROWS : (g + 1) * ROWS] = bits_of(
                        lhs[s, g, pl.ds(base + w, 1), :], mask, F8
                    )
            at = pl.ds(pl.multiple_of(i * TILE, TILE), TILE)
            part = jnp.dot(w_lhs[...], w_rhs[...], preferred_element_type=jnp.float32)
            if first:
                acc[at, :] = part
            else:
                acc[at, :] += part

    @pl.when(off)
    def _():
        for s in range(2):
            copy(own, rhs.at[s], send.at[0], rhs_sem.at[s], row, col).wait_recv()
            unpack_rhs(rhs.at[s])
            copy(own, lhs.at[s, h], send.at[0], lhs_sem.at[s], row, col).wait_recv()
            relay(s).start()
            copy(own, lhs.at[s, 1 - h], send.at[0], relay_sem.at[s], row, col).wait_recv()
            product(s, s == 0)
        copy(own, lhs.at[2, h], send.at[0], lhs_sem.at[2], row, col).wait_recv()
        relay(2).start()

    @pl.when(diag)
    def _():
        acc[...] = jnp.zeros_like(acc)

    unpack_rhs(own)
    copy(own, lhs.at[2, 1 - h], send.at[0], relay_sem.at[2], row, col).wait_recv()
    product(2, False)

    zero = jnp.zeros((1, ROWS), jnp.float32)

    def fold(i, carry):
        closed, degree = carry
        base = pl.multiple_of(i * 8, 8)
        for q in range(2):
            sums = []
            for w in range(4):
                at = pl.multiple_of(i * 256 + q * 128 + w * 32, 32)
                bit = bits_of(own[pl.ds(base + q * 4 + w, 1), :], mask, jnp.float32)
                val = bit * acc[pl.ds(at, 32), :]
                closed = closed + jnp.sum(val.reshape(4, 8, ROWS), axis=0)
                degree = degree + jnp.sum(bit.reshape(4, 8, ROWS), axis=0)
                sums.append(sum(val[:, k * 128 : (k + 1) * 128] for k in range(5)))
            across = jnp.concatenate(sums, axis=0).T
            part_col[2 * i + q, :, :] = 2.0 * jnp.sum(across, axis=0, keepdims=True)
        return closed, degree

    closed, degree = lax.fori_loop(
        0, 5, fold, (jnp.zeros((8, ROWS), jnp.float32), jnp.zeros((8, ROWS), jnp.float32))
    )
    closed = jnp.sum(closed, axis=0, keepdims=True)
    degree = jnp.sum(degree, axis=0, keepdims=True)
    for k in range(5):
        part_row[k, :, :] = closed[:, k * 128 : (k + 1) * 128]
        part_row[5 + k, :, :] = degree[:, k * 128 : (k + 1) * 128]

    give_row = copy(part_row, red_row.at[C], send.at[10], row_sem.at[C], row, R)
    give_col = [
        copy(
            part_col.at[pl.ds(5 * g, 5)], red_col.at[R, h], send.at[11 + g],
            col_sem.at[R, h], 2 * C + g, C,
        )
        for g in range(2)
    ]

    @pl.when(off)
    def _():
        give_row.start()
        for c in give_col:
            c.start()
        for c in offers:
            c.wait_send()
        for s in range(2):
            relay(s).wait_send()
        relay(2).wait_send()
        give_row.wait_send()
        for c in give_col:
            c.wait_send()

    def tell(i):
        to = (row * 8 + col + i) % 128
        return copy(mine, every.at[row], all_send.at[i], all_sem.at[row], to // 8, to % 8)

    @pl.when(diag)
    def _():
        for c in spread:
            c.wait_send()
        relay(2).wait_send()
        tot = part_row[...]

        def add(i, tot):
            o = (R + i) % 8
            copy(part_row, red_row.at[o], send.at[0], row_sem.at[o], row, col).wait_recv()
            tot = tot + red_row[o]
            both = jnp.zeros((5, 1, 128), jnp.float32)
            for g in range(2):
                copy(
                    part_col.at[pl.ds(0, 5)], red_col.at[o, g], send.at[0],
                    col_sem.at[o, g], row, col,
                ).wait_recv()
                both = both + red_col[o, g]
            return tot + jnp.concatenate([both, jnp.zeros_like(both)], axis=0)

        tot = lax.fori_loop(1, 8, add, tot)
        total, deg = tot[:5, 0, :], tot[5:, 0, :]
        wedges = jnp.maximum(deg * (deg - 1.0), 1.0)
        mine[0:5, :] = total / wedges
        mine[5:6, :] = jnp.sum(total, axis=0, keepdims=True)
        mine[6:7, :] = jnp.sum(wedges, axis=0, keepdims=True)
        mine[7:8, :] = jnp.zeros((1, 128), jnp.float32)
        every[row] = mine[...]

        @pl.loop(1, 128)
        def _(i):
            tell(i).start()

    def arrived(b):
        @pl.when((R != C) | (row != b))
        def _():
            copy(mine, every.at[b], all_send.at[0], all_sem.at[b], row, col).wait_recv()

    for b in range(16):
        arrived(b)

    want = jnp.broadcast_to(rel[...], (8, 128))
    block, rest = want // ROWS, want % ROWS
    line, lane = rest // 128, rest % 128
    here = lax.broadcasted_iota(I32, (8, 128), 0) == line
    found = jnp.zeros((8, 128), jnp.float32)
    sums = jnp.zeros((8, 128), jnp.float32)
    for b in range(16):
        tile = every[b]
        sums = sums + tile
        got = jnp.take_along_axis(tile, lane, axis=1)
        found = found + jnp.where(here & (block == b), got, 0.0)
    ratio = jnp.sum(sums[5:6, :], axis=1, keepdims=True) / jnp.sum(
        sums[6:7, :], axis=1, keepdims=True
    )
    out[0:1, :] = jnp.sum(found, axis=0, keepdims=True)
    out[1:2, :] = jnp.broadcast_to(ratio, (1, 128))

    @pl.when(diag)
    def _():
        @pl.loop(1, 128)
        def _(i):
            tell(i).wait_send()


def body(adjacency, relabel):
    f32 = jnp.float32
    dma = pltpu.SemaphoreType.DMA
    wanted = jnp.pad(relabel, (0, 48))[None, :]
    out = pl.pallas_call(
        kernel,
        out_shape=jax.ShapeDtypeStruct((2, 128), f32),
        in_specs=[pl.BlockSpec(memory_space=pltpu.VMEM)] * 2,
        out_specs=pl.BlockSpec(memory_space=pltpu.VMEM),
        scratch_shapes=[
            pltpu.VMEM((WORDS, ROWS), I32),
            pltpu.VMEM((2, WORDS, ROWS), I32),
            pltpu.VMEM((3, 2, WORDS, ROWS), I32),
            pltpu.VMEM((WIDE, ROWS), F8),
            pltpu.VMEM((TILE, WIDE), F8),
            pltpu.VMEM((WIDE, ROWS), f32),
            pltpu.VMEM((10, 1, 128), f32),
            pltpu.VMEM((10, 1, 128), f32),
            pltpu.VMEM((8, 10, 1, 128), f32),
            pltpu.VMEM((8, 2, 5, 1, 128), f32),
            pltpu.VMEM((8, 128), f32),
            pltpu.VMEM((16, 8, 128), f32),
            dma((13,)),
            dma((2,)),
            dma((3,)),
            dma((3,)),
            dma((8,)),
            dma((8, 2)),
            dma((128,)),
            dma((16,)),
        ],
        compiler_params=pltpu.CompilerParams(
            collective_id=0, has_side_effects=True, vmem_limit_bytes=48 * 2**20
        ),
    )(adjacency, wanted)
    return out[0, :80], out[1, 0]


def solution(mesh):
    placed = (P("row", "col"), P(("row", "col")))
    return jax.shard_map(
        body, mesh=mesh, in_specs=placed, out_specs=(P(("row", "col")), P()), check_vma=False
    )
```

```python
import jax
import jax.numpy as jnp
from jax import lax
from jax.experimental import pallas as pl
from jax.experimental.pallas import tpu as pltpu
from jax.sharding import PartitionSpec as P

SENDS_A = (
    148879702, 171848828, 263397976, 238957692, 196967528, 255419081, 162998856, 188054224,
    180303480, 140426066, 247412344, 254943324, 263741645, 188513900, 196376788, 154544204,
    246620752, 255602804, 207534942, 188493940, 146221632, 171409112, 180320352, 238773953,
    264057456, 238166100, 196948592, 215988570, 179731676, 137766980, 247096517, 171866724,
    255029992, 247098073, 196289112, 146367552, 224112966, 229669992, 154889812, 205403244,
    238774493, 263352556, 137913924, 187834460, 221347436, 232436546, 213857896, 163212368,
    179511888, 163275840, 146568928, 263745233, 137981524, 222048356, 207270734, 213022816,
    154822212, 171057236, 255421653, 138245348, 230503008, 146304080, 204700260, 215724362,
)
SENDS_B = (
    2012494, 0, 0, 0, 0, 0, 0, 0,
    0, 2078538, 0, 0, 0, 0, 0, 0,
    0, 0, 1877830, 0, 0, 0, 0, 0,
    0, 0, 0, 1942850, 0, 0, 0, 0,
    0, 0, 0, 0, 2010966, 0, 0, 0,
    0, 0, 0, 0, 0, 2075986, 0, 0,
    0, 0, 0, 0, 0, 0, 1551218, 0,
    0, 0, 0, 0, 0, 0, 0, 1485174,
)
KIND = (
    0, 1, 0, 1, 0, 1, 0, 0,
    1, 0, 1, 0, 1, 0, 0, 0,
    0, 1, 0, 1, 0, 0, 0, 1,
    1, 0, 1, 0, 0, 0, 1, 0,
    0, 1, 0, 0, 0, 1, 0, 1,
    1, 0, 0, 0, 1, 0, 1, 0,
    0, 0, 0, 1, 0, 1, 0, 1,
    0, 0, 1, 0, 1, 0, 1, 0,
)

F8 = jnp.float8_e4m3fn
I32 = jnp.int32
F32 = jnp.float32
WORDS, ROWS, WIDE = 40, 640, 1280
TALL = 640
X, Y, Z = 4, 4, 4


def look_up(table, d):
    return sum(jnp.where(d == i, I32(v), I32(0)) for i, v in enumerate(table) if v)


def bit_set(row, mask):
    return (jnp.broadcast_to(row, (32, row.shape[1])) & mask) != 0


def ones(row, mask):
    return jnp.where(bit_set(row, mask), 1.0, 0.0).astype(F8)


def kernel(
    adj, rel, out, ratio_out,
    own, inbox, w_rhs, w_lhs, acc, part_row, part_col, red_row, red_col, mine, every, want_ref,
    adj_sem, send, relay_sem, in_sem, row_sem, col_sem, all_send, all_sem,
):
    row, col = lax.axis_index("row"), lax.axis_index("col")
    R, C, h = row // 2, col, row % 2
    g = 1 - h
    diag, off = R == C, R != C
    fetch = pltpu.make_async_copy(adj, own, adj_sem)
    fetch.start()

    barrier = pltpu.get_barrier_semaphore()

    def hello(r, c):
        pl.semaphore_signal(barrier, inc=1, device_id={"row": r, "col": c})

    for i in range(1, 8):
        hello(row, (C + i) % 8)
        hello(2 * ((R + i) % 8) + h, C)
    hello(2 * R + g, C)

    place = R * 8 + C
    kind = look_up(KIND, place)
    codes_a, codes_b = look_up(SENDS_A, place), look_up(SENDS_B, place)
    lhs_is_own = diag | (kind == 1)
    rhs_is_own = kind == 0

    mask = jnp.left_shift(I32(1), lax.broadcasted_iota(I32, (32, ROWS), 0))
    fetch.wait()

    @pl.when(lhs_is_own)
    def _():
        inbox[7 + h] = own[...]

    @pl.when(rhs_is_own)
    def _():
        inbox[2] = own[...]

    pl.semaphore_wait(barrier, 15)

    def copy(src, dst, ssem, rsem, r, c):
        return pltpu.make_async_remote_copy(
            src_ref=src, dst_ref=dst, send_sem=ssem, recv_sem=rsem,
            device_id={"row": r, "col": c},
        )

    def offer(i):
        code = (codes_a if i < 4 else codes_b) // (128 ** (i % 4)) % 128
        slot, to, down = code % 4, code // 4 % 8, code // 32 % 2
        box = jnp.where(down == 1, 3 + 2 * slot + h, slot)
        r = jnp.where(down == 1, 2 * to + h, row)
        c = jnp.where(down == 1, col, to)
        return code >= 64, copy(own, inbox.at[box], send.at[i], in_sem.at[box], r, c)

    for i in range(7):
        there, c = offer(i)
        pl.when(there)(c.start)

    def relay(s):
        box = 3 + 2 * s + h
        return copy(inbox.at[box], inbox.at[box], relay_sem.at[s], in_sem.at[box], 2 * R + g, C)

    def arrived(box):
        copy(own, inbox.at[box], send.at[0], in_sem.at[box], row, col).wait_recv()

    def pass_on(s):
        @pl.when((s < 2) | jnp.logical_not(lhs_is_own))
        def _():
            arrived(3 + 2 * s + h)

        relay(s).start()

    first = jnp.where(diag, 2, 0)
    pass_on(first)
    acc[...] = jnp.zeros_like(acc)

    def unpack(box, to):
        @pl.loop(0, 5)
        def _(i):
            base = pl.multiple_of(i * 8, 8)
            for w in range(8):
                to(
                    pl.ds(pl.multiple_of(i * 256 + w * 32, 32), 32),
                    ones(inbox[box, pl.ds(base + w, 1), :], mask),
                )

    def to_rhs(at, value):
        w_rhs[at, :] = value

    def to_lhs(k):
        def put(at, value):
            w_lhs[at, k * ROWS : (k + 1) * ROWS] = value
        return put

    @pl.loop(first, 3)
    def _(s):
        @pl.when((s < 2) | jnp.logical_not(rhs_is_own))
        def _():
            arrived(s)

        unpack(s, to_rhs)

        @pl.when(s < 2)
        def _():
            pass_on(s + 1)

        def half(k):
            @pl.when(k == g)
            def _():
                arrived(3 + 2 * s + k)

            unpack(3 + 2 * s + k, to_lhs(k))

        half(0)
        half(1)

        @pl.loop(0, WIDE // TALL)
        def _(i):
            at = pl.ds(pl.multiple_of(i * TALL, TALL), TALL)
            acc[at, :] += jnp.dot(w_lhs[at, :], w_rhs[...], preferred_element_type=F32)

    def fold(i, carry):
        closed, degree = carry
        base = pl.multiple_of(i * 8, 8)
        for q in range(2):
            sums = []
            for w in range(4):
                at = pl.multiple_of(i * 256 + q * 128 + w * 32, 32)
                bit = bit_set(own[pl.ds(base + q * 4 + w, 1), :], mask)
                val = jnp.where(bit, acc[pl.ds(at, 32), :], 0.0)
                one = jnp.where(bit, 1.0, 0.0)
                closed = closed + jnp.sum(val.reshape(4, 8, ROWS), axis=0)
                degree = degree + jnp.sum(one.reshape(4, 8, ROWS), axis=0)
                sums.append(sum(val[:, k * 128 : (k + 1) * 128] for k in range(5)))
            across = jnp.concatenate(sums, axis=0).T
            part_col[2 * i + q, :, :] = jnp.sum(across, axis=0, keepdims=True)
        return closed, degree

    zeros = jnp.zeros((8, ROWS), F32)
    closed, degree = lax.fori_loop(0, 5, fold, (zeros, zeros))
    once_more = kind.astype(F32)
    closed = jnp.sum(closed, axis=0, keepdims=True) * (1.0 + once_more)
    degree = jnp.sum(degree, axis=0, keepdims=True)
    part_col[...] = part_col[...] * (2.0 - once_more)
    for k in range(5):
        part_row[k, :, :] = closed[:, k * 128 : (k + 1) * 128]
        part_row[5 + k, :, :] = degree[:, k * 128 : (k + 1) * 128]

    give_row = copy(part_row, red_row.at[C], send.at[7], row_sem.at[C], row, R)
    give_col = [
        copy(
            part_col.at[pl.ds(5 * k, 5)], red_col.at[R, h], send.at[8 + k],
            col_sem.at[R, h], 2 * C + k, C,
        )
        for k in range(2)
    ]

    @pl.when(off)
    def _():
        give_row.start()
        for c in give_col:
            c.start()

    def tell(dx, i, k):
        x, y, z = C // 4 * 2 + R % 2, R // 2, C % 4
        x, y, z = (x + dx) % X, (y + 2 + i // 4) % Y, (z + 2 + i % 4) % Z
        r, c = y * 4 + x % 2 * 2 + k, x // 2 * 4 + z
        return copy(mine, every.at[row], all_send.at[r * 8 + c], all_sem.at[row], r, c)

    HOME = 10

    def for_all(act):
        for dx in (2, 1, 3, 0):
            @pl.loop(0, 16)
            def _(i):
                @pl.when((i != HOME) | (dx != 0))
                def _():
                    for k in range(2):
                        act(tell(dx, i, k))
        act(tell(0, HOME, g))

    @pl.when(diag)
    def _():
        tot = part_row[...]

        def add(i, tot):
            o = (R + i) % 8
            copy(part_row, red_row.at[o], send.at[0], row_sem.at[o], row, col).wait_recv()
            tot = tot + red_row[o]
            both = jnp.zeros((5, 1, 128), F32)
            for k in range(2):
                copy(
                    part_col.at[pl.ds(0, 5)], red_col.at[o, k], send.at[0],
                    col_sem.at[o, k], row, col,
                ).wait_recv()
                both = both + red_col[o, k]
            return tot + jnp.concatenate([both, jnp.zeros_like(both)], axis=0)

        tot = lax.fori_loop(1, 8, add, tot)
        total, deg = tot[:5, 0, :], tot[5:, 0, :]
        wedges = jnp.maximum(deg * (deg - 1.0), 1.0)
        mine[0:5, :] = total / wedges
        low = lax.broadcasted_iota(I32, (1, 128), 1) < 64
        both = []
        for v in (total, wedges):
            v = jnp.sum(v, axis=0, keepdims=True)
            both.append(v + pltpu.roll(v, 64, 1))
        mine[5:6, :] = jnp.where(low, both[0], both[1])
        every[row] = mine[...]
        for_all(lambda c: c.start())

    want_ref[...] = jnp.zeros_like(want_ref)
    want_ref[:, 0:80] = rel[...]
    want = jnp.broadcast_to(want_ref[...], (6, 128))
    block, rest = want // ROWS, want % ROWS
    line, lane = rest // 128, rest % 128
    here = lax.broadcasted_iota(I32, (6, 128), 0) == line

    for i in range(7):
        there, c = offer(i)
        pl.when(there)(c.wait_send)

    @pl.loop(first, 3)
    def _(s):
        relay(s).wait_send()

    @pl.when(off)
    def _():
        give_row.wait_send()
        for c in give_col:
            c.wait_send()

    found = jnp.zeros((6, 128), F32)
    sums = jnp.zeros((1, 128), F32)
    for b in range(16):
        @pl.when(off | (row != b))
        def _():
            copy(mine, every.at[b], all_send.at[0], all_sem.at[b], row, col).wait_recv()

        tile = every[b]
        sums = sums + tile[5:6, :]
        got = jnp.take_along_axis(tile, lane, axis=1)
        found = found + jnp.where(here & (block == b), got, 0.0)
    low = lax.broadcasted_iota(I32, (1, 128), 1) < 64
    top = jnp.sum(jnp.where(low, sums, 0.0), axis=1, keepdims=True)
    bottom = jnp.sum(jnp.where(low, 0.0, sums), axis=1, keepdims=True)
    ratio_out[...] = top / bottom
    out[...] = jnp.sum(found, axis=0, keepdims=True)[:, 0:80]

    @pl.when(diag)
    def _():
        for_all(lambda c: c.wait_send())


def body(adjacency, relabel):
    dma = pltpu.SemaphoreType.DMA
    vmem = pltpu.VMEM
    out, ratio = pl.pallas_call(
        kernel,
        out_shape=(jax.ShapeDtypeStruct((1, 80), F32), jax.ShapeDtypeStruct((1, 1), F32)),
        in_specs=[pl.BlockSpec(memory_space=pl.ANY), pl.BlockSpec(memory_space=vmem)],
        out_specs=[pl.BlockSpec(memory_space=vmem)] * 2,
        scratch_shapes=[
            vmem((WORDS, ROWS), I32),
            vmem((9, WORDS, ROWS), I32),
            vmem((WIDE, ROWS), F8),
            vmem((WIDE, WIDE), F8),
            vmem((WIDE, ROWS), F32),
            vmem((10, 1, 128), F32),
            vmem((10, 1, 128), F32),
            vmem((8, 10, 1, 128), F32),
            vmem((8, 2, 5, 1, 128), F32),
            vmem((6, 128), F32),
            vmem((16, 6, 128), F32),
            vmem((1, 128), I32),
            dma,
            dma((10,)),
            dma((3,)),
            dma((9,)),
            dma((8,)),
            dma((8, 2)),
            dma((128,)),
            dma((16,)),
        ],
        compiler_params=pltpu.CompilerParams(
            collective_id=0, has_side_effects=True, vmem_limit_bytes=48 * 2**20
        ),
    )(adjacency.T, relabel[None, :])
    return out[0], ratio[0, 0]


def solution(mesh):
    placed = (P("row", "col"), P(("row", "col")))
    return jax.shard_map(
        body, mesh=mesh, in_specs=placed, out_specs=(P(("row", "col")), P()), check_vma=False
    )
```

```python
import jax
import jax.numpy as jnp
from jax import lax
from jax.experimental import pallas as pl
from jax.experimental.pallas import tpu as pltpu
from jax.sharding import PartitionSpec as P

SENDS_A = (
    257605490, 171605116, 163537496, 1866856, 197031157, 146367608, 179465804, 229911156,
    180303480, 266059126, 1801844, 155082844, 138375372, 230452348, 221587568, 187983560,
    146040436, 238973044, 199012726, 205355132, 137833028, 1539792, 180121724, 162930800,
    247427696, 154493040, 247036152, 190690162, 1469048, 137766980, 146220148, 171801828,
    163476709, 180186216, 146171484, 263201380, 257603426, 138310764, 196831816, 1604712,
    171734748, 263742572, 254877792, 154169048, 146749032, 266057062, 2061924, 188377164,
    171123284, 1275584, 146307180, 196225120, 179334756, 205158500, 165458278, 238645356,
    1204840, 171057236, 179514468, 137983220, 213613152, 187787360, 247034088, 157135714,
)
SENDS_B = (
    1286998, 0, 0, 0, 0, 0, 0, 89,
    0, 1220946, 0, 0, 0, 0, 93, 0,
    0, 89, 1287002, 0, 0, 0, 0, 0,
    93, 0, 0, 1220958, 0, 0, 0, 0,
    0, 0, 0, 73, 1551174, 0, 0, 0,
    0, 0, 77, 0, 0, 1485122, 0, 0,
    0, 0, 0, 0, 0, 73, 1551178, 0,
    0, 0, 0, 0, 77, 0, 0, 1485134,
)
KIND = (
    0, 1, 0, 1, 0, 1, 0, 0,
    1, 0, 1, 0, 1, 0, 0, 0,
    0, 1, 0, 1, 0, 0, 1, 1,
    1, 0, 1, 0, 0, 0, 1, 1,
    0, 1, 0, 0, 0, 1, 0, 1,
    1, 0, 0, 0, 1, 0, 1, 0,
    0, 0, 1, 1, 0, 1, 0, 1,
    0, 0, 1, 1, 1, 0, 1, 0,
)

F8 = jnp.float8_e4m3fn
I32 = jnp.int32
F32 = jnp.float32
WORDS, ROWS, WIDE = 40, 640, 1280


def look_up(table, d):
    return sum(jnp.where(d == i, I32(v), I32(0)) for i, v in enumerate(table) if v)


def halves(words, top):
    twice = jnp.concatenate([words, words], axis=0)
    return jnp.where(top, twice & 0xFFFF, lax.shift_right_logical(twice, 16))


def unpacked(words, top, bits):
    part = halves(words, top)
    part = jnp.concatenate([part, part], axis=0).astype(jnp.int16)
    one, none = jnp.bfloat16(1), jnp.bfloat16(0)
    rows = [jnp.where((part & b) != 0, one, none) for b in bits]
    return [jnp.concatenate(rows[2 * j : 2 * j + 2], axis=0).astype(F8) for j in range(4)]


def kernel(
    adj, rel, out, ratio_out,
    plain, own, inbox, w_rhs, w_lhs, acc, part_row, part_col, red_row, red_col, mine, every, want_ref,
    adj_sem, send, relay_sem, in_sem, row_sem, col_sem, all_send, all_sem,
):
    row, col = lax.axis_index("row"), lax.axis_index("col")
    R, C, h = row // 2, col, row % 2
    g = 1 - h
    diag, off = R == C, R != C
    fetch = pltpu.make_async_copy(adj, plain, adj_sem)
    fetch.start()

    barrier = pltpu.get_barrier_semaphore()

    def hello(r, c):
        pl.semaphore_signal(barrier, inc=1, device_id={"row": r, "col": c})

    for i in range(1, 8):
        hello(row, (C + i) % 8)
        hello(2 * ((R + i) % 8) + h, C)
    hello(2 * R + g, C)

    place = R * 8 + C
    kind = look_up(KIND, place)
    codes_a, codes_b = look_up(SENDS_A, place), look_up(SENDS_B, place)
    lhs_is_own = diag | (kind == 1)
    rhs_is_own = kind == 0

    p = lax.broadcasted_iota(I32, (8, 128), 1)
    column = 32 * (p % 4) + 16 * (p // 4 % 2) + p // 8
    fetch.wait()

    @pl.loop(0, 5)
    def _(i):
        at = pl.ds(pl.multiple_of(i * 8, 8), 8)
        for k in range(5):
            lanes = slice(k * 128, (k + 1) * 128)
            own[at, lanes] = jnp.take_along_axis(plain[at, lanes], column, axis=1)


    @pl.when(lhs_is_own)
    def _():
        inbox[7 + h] = own[...]

    @pl.when(rhs_is_own)
    def _():
        inbox[2] = own[...]

    pl.semaphore_wait(barrier, 15)

    def copy(src, dst, ssem, rsem, r, c):
        return pltpu.make_async_remote_copy(
            src_ref=src, dst_ref=dst, send_sem=ssem, recv_sem=rsem,
            device_id={"row": r, "col": c},
        )

    def offer(i):
        code = (codes_a if i < 4 else codes_b) // (128 ** (i % 4)) % 128
        slot, to, down = code % 4, code // 4 % 8, code // 32 % 2
        box = jnp.where(down == 1, 3 + 2 * slot + h, slot)
        r = jnp.where(down == 1, 2 * to + h, row)
        c = jnp.where(down == 1, col, to)
        return code >= 64, slot, copy(own, inbox.at[box], send.at[i], in_sem.at[box], r, c)

    for i in range(7):
        there, slot, c = offer(i)
        pl.when(there & (slot != 1))(c.start)

    def relay(s):
        box = 3 + 2 * s + h
        return copy(inbox.at[box], inbox.at[box], relay_sem.at[s], in_sem.at[box], 2 * R + g, C)

    def arrived(box):
        copy(own, inbox.at[box], send.at[0], in_sem.at[box], row, col).wait_recv()

    def pass_on(s):
        @pl.when((s < 2) | jnp.logical_not(lhs_is_own))
        def _():
            arrived(3 + 2 * s + h)

        relay(s).start()

    first = jnp.where(diag, 2, 0)
    acc[...] = jnp.zeros_like(acc)
    pass_on(first)

    for i in range(5):
        there, slot, c = offer(i)
        pl.when(there & (slot == 0))(c.wait_send)
    for i in range(5):
        there, slot, c = offer(i)
        pl.when(there & (slot == 1))(c.start)

    top = lax.broadcasted_iota(I32, (8, 128), 0) < 4
    upper = lax.broadcasted_iota(I32, (16, 128), 0) < 8
    bits = [
        jnp.where(upper, I32(1 << k), I32(1 << (k + 1) if k < 14 else -32768)).astype(jnp.int16)
        for k in range(0, 16, 2)
    ]

    def unpack(box, i, put):
        for k in range(5):
            words = inbox[box, pl.ds(pl.multiple_of(i * 8, 8), 8), k * 128 : (k + 1) * 128]
            for q in range(2):
                for j, piece in enumerate(unpacked(words[4 * q : 4 * q + 4], top, bits)):
                    put(q * 128 + j * 32, k * 128, piece)

    def product(lo, hi):
        for k in range(2):
            for i in range(lo, hi):
                def put(r, c, piece):
                    w_lhs[i * 256 + r : i * 256 + r + 32, k * ROWS + c : k * ROWS + c + 128] = piece
                unpack(3 + 2 * s_now[0] + k, i, put)
        at = slice(lo * 256, hi * 256)
        acc[at, :] += jnp.dot(w_lhs[at, :], w_rhs[...], preferred_element_type=F32)

    s_now = [None]

    @pl.loop(first, 3)
    def _(s):
        @pl.when((s < 2) | jnp.logical_not(rhs_is_own))
        def _():
            arrived(s)

        @pl.loop(0, 5)
        def _(i):
            def put(r, c, piece):
                w_rhs[pl.ds(pl.multiple_of(i * 256 + r, 32), 32), c : c + 128] = piece
            unpack(s, i, put)

        arrived(3 + 2 * s + g)
        s_now[0] = s
        product(0, 3)

        @pl.when(s < 2)
        def _():
            pass_on(s + 1)

        product(3, 5)

    def fold(i, closed):
        words = own[pl.ds(pl.multiple_of(i * 8, 8), 8), :]
        for q in range(2):
            part = halves(words[4 * q : 4 * q + 4], wide_top)
            sums = []
            for k in range(16):
                at = pl.multiple_of(i * 256 + q * 128 + k * 8, 8)
                val = jnp.where((part & (1 << k)) != 0, acc[pl.ds(at, 8), :], 0.0)
                closed = closed + val
                sums.append(sum(val[:, k * 128 : (k + 1) * 128] for k in range(5)))
            across = jnp.concatenate(sums, axis=0).T
            part_col[2 * i + q, :, :] = jnp.sum(across, axis=0, keepdims=True)
        return closed

    wide_top = lax.broadcasted_iota(I32, (8, ROWS), 0) < 4
    degree = jnp.sum(lax.population_count(own[...]), axis=0, keepdims=True).astype(F32)
    closed = lax.fori_loop(0, 5, fold, jnp.zeros((8, ROWS), F32))
    once_more = kind.astype(F32)
    closed = jnp.sum(closed, axis=0, keepdims=True) * (1.0 + once_more)
    part_col[...] = part_col[...] * (2.0 - once_more)
    for k in range(5):
        part_row[k, :, :] = closed[:, k * 128 : (k + 1) * 128]
        part_row[5 + k, :, :] = degree[:, k * 128 : (k + 1) * 128]

    give_row = copy(part_row, red_row.at[C], send.at[7], row_sem.at[C], row, R)
    give_col = [
        copy(
            part_col.at[pl.ds(5 * k, 5)], red_col.at[R, h], send.at[8 + k],
            col_sem.at[R, h], 2 * C + k, C,
        )
        for k in range(2)
    ]

    @pl.when(off)
    def _():
        give_row.start()
        for c in give_col:
            c.start()

    def tell(r, c):
        return copy(mine, every.at[row], all_send.at[r * 8 + c], all_sem.at[row], r, c)

    def for_all(act):
        for x in (0, 1, 3, 2):
            for y in (0, 1, 3, 2):
                @pl.loop(0, 8)
                def _(i):
                    r, c = y * 4 + x % 2 * 2 + i % 2, x // 2 * 4 + i // 2

                    @pl.when((r != row) | (c != col))
                    def _():
                        act(tell(r, c))

    @pl.when(diag)
    def _():
        tot = part_row[...]

        def add(i, tot):
            o = (R + i) % 8
            copy(part_row, red_row.at[o], send.at[0], row_sem.at[o], row, col).wait_recv()
            tot = tot + red_row[o]
            both = jnp.zeros((5, 1, 128), F32)
            for k in range(2):
                copy(
                    part_col.at[pl.ds(0, 5)], red_col.at[o, k], send.at[0],
                    col_sem.at[o, k], row, col,
                ).wait_recv()
                both = both + red_col[o, k]
            return tot + jnp.concatenate([both, jnp.zeros_like(both)], axis=0)

        tot = lax.fori_loop(1, 8, add, tot)
        total, deg = tot[:5, 0, :], tot[5:, 0, :]
        wedges = jnp.maximum(deg * (deg - 1.0), 1.0)
        mine[0:5, :] = total / wedges
        low = lax.broadcasted_iota(I32, (1, 128), 1) < 64
        both = []
        for v in (total, wedges):
            v = jnp.sum(v, axis=0, keepdims=True)
            both.append(v + pltpu.roll(v, 64, 1))
        mine[5:6, :] = jnp.where(low, both[0], both[1])
        every[row] = mine[...]
        for_all(lambda c: c.start())

    want_ref[...] = jnp.zeros_like(want_ref)
    want_ref[:, 0:80] = rel[...]
    want = jnp.broadcast_to(want_ref[...], (6, 128))
    block, rest = want // ROWS, want % ROWS
    line, lane = rest // 128, rest % 128
    lane = 8 * (lane % 16) + 4 * (lane // 16 % 2) + lane // 32
    here = lax.broadcasted_iota(I32, (6, 128), 0) == line

    for i in range(7):
        there, slot, c = offer(i)
        pl.when(there & (slot != 0))(c.wait_send)

    @pl.loop(first, 3)
    def _(s):
        relay(s).wait_send()

    @pl.when(off)
    def _():
        give_row.wait_send()
        for c in give_col:
            c.wait_send()

    found = jnp.zeros((6, 128), F32)
    sums = jnp.zeros((1, 128), F32)
    for b in range(16):
        @pl.when(off | (row != b))
        def _():
            copy(mine, every.at[b], all_send.at[0], all_sem.at[b], row, col).wait_recv()

        tile = every[b]
        sums = sums + tile[5:6, :]
        got = jnp.take_along_axis(tile, lane, axis=1)
        found = found + jnp.where(here & (block == b), got, 0.0)
    low = lax.broadcasted_iota(I32, (1, 128), 1) < 64
    top = jnp.sum(jnp.where(low, sums, 0.0), axis=1, keepdims=True)
    bottom = jnp.sum(jnp.where(low, 0.0, sums), axis=1, keepdims=True)
    ratio_out[...] = top / bottom
    out[...] = jnp.sum(found, axis=0, keepdims=True)[:, 0:80]

    @pl.when(diag)
    def _():
        for_all(lambda c: c.wait_send())


def body(adjacency, relabel):
    dma = pltpu.SemaphoreType.DMA
    vmem = pltpu.VMEM
    out, ratio = pl.pallas_call(
        kernel,
        out_shape=(jax.ShapeDtypeStruct((1, 80), F32), jax.ShapeDtypeStruct((1, 1), F32)),
        in_specs=[pl.BlockSpec(memory_space=pl.ANY), pl.BlockSpec(memory_space=vmem)],
        out_specs=[pl.BlockSpec(memory_space=vmem)] * 2,
        scratch_shapes=[
            vmem((WORDS, ROWS), I32),
            vmem((WORDS, ROWS), I32),
            vmem((9, WORDS, ROWS), I32),
            vmem((WIDE, ROWS), F8),
            vmem((WIDE, WIDE), F8),
            vmem((WIDE, ROWS), F32),
            vmem((10, 1, 128), F32),
            vmem((10, 1, 128), F32),
            vmem((8, 10, 1, 128), F32),
            vmem((8, 2, 5, 1, 128), F32),
            vmem((6, 128), F32),
            vmem((16, 6, 128), F32),
            vmem((1, 128), I32),
            dma,
            dma((10,)),
            dma((3,)),
            dma((9,)),
            dma((8,)),
            dma((8, 2)),
            dma((128,)),
            dma((16,)),
        ],
        compiler_params=pltpu.CompilerParams(
            collective_id=0, has_side_effects=True, vmem_limit_bytes=67043328
        ),
    )(adjacency.T, relabel[None, :])
    return out[0], ratio[0, 0]


def solution(mesh):
    placed = (P("row", "col"), P(("row", "col")))
    return jax.shard_map(
        body, mesh=mesh, in_specs=placed, out_specs=(P(("row", "col")), P()), check_vma=False
    )
```

```python
import jax
import jax.numpy as jnp
from jax import lax
from jax.experimental import pallas as pl
from jax.experimental.pallas import tpu as pltpu
from jax.sharding import PartitionSpec as P

SENDS_A = (
    257605490, 171605116, 163537496, 1866856, 197031157, 146367608, 179465804, 229911156,
    180303480, 266059126, 1801844, 155082844, 138375372, 230452348, 221587568, 187983560,
    146040436, 238973044, 199012726, 205355132, 137833028, 1539792, 180121724, 162930800,
    247427696, 154493040, 247036152, 190690162, 1469048, 137766980, 146220148, 171801828,
    163476709, 180186216, 146171484, 263201380, 257603426, 138310764, 196831816, 1604712,
    171734748, 263742572, 254877792, 154169048, 146749032, 266057062, 2061924, 188377164,
    171123284, 1275584, 146307180, 196225120, 179334756, 205158500, 165458278, 238645356,
    1204840, 171057236, 179514468, 137983220, 213613152, 187787360, 247034088, 157135714,
)
SENDS_B = (
    1286998, 0, 0, 0, 0, 0, 0, 89,
    0, 1220946, 0, 0, 0, 0, 93, 0,
    0, 89, 1287002, 0, 0, 0, 0, 0,
    93, 0, 0, 1220958, 0, 0, 0, 0,
    0, 0, 0, 73, 1551174, 0, 0, 0,
    0, 0, 77, 0, 0, 1485122, 0, 0,
    0, 0, 0, 0, 0, 73, 1551178, 0,
    0, 0, 0, 0, 77, 0, 0, 1485134,
)
KIND = (
    0, 1, 0, 1, 0, 1, 0, 0,
    1, 0, 1, 0, 1, 0, 0, 0,
    0, 1, 0, 1, 0, 0, 1, 1,
    1, 0, 1, 0, 0, 0, 1, 1,
    0, 1, 0, 0, 0, 1, 0, 1,
    1, 0, 0, 0, 1, 0, 1, 0,
    0, 0, 1, 1, 0, 1, 0, 1,
    0, 0, 1, 1, 1, 0, 1, 0,
)

F8 = jnp.float8_e4m3fn
I32 = jnp.int32
F32 = jnp.float32
WORDS, ROWS, WIDE = 40, 640, 1280


def look_up(table, d):
    return sum(jnp.where(d == i, I32(v), I32(0)) for i, v in enumerate(table) if v)


def halves(words, top):
    twice = jnp.concatenate([words, words], axis=0)
    return jnp.where(top, twice & 0xFFFF, lax.shift_right_logical(twice, 16))


def unpacked(words, top, bits):
    part = halves(words, top)
    part = jnp.concatenate([part, part], axis=0).astype(jnp.int16)
    one, none = jnp.bfloat16(1), jnp.bfloat16(0)
    rows = [jnp.where((part & b) != 0, one, none) for b in bits]
    return [jnp.concatenate(rows[2 * j : 2 * j + 2], axis=0).astype(F8) for j in range(4)]


def kernel(
    adj, rel, out, ratio_out,
    plain, own, inbox, w_rhs, w_lhs, acc, part_row, part_col, red_row, red_col, mine, every, want_ref,
    adj_sem, send, relay_sem, in_sem, row_sem, col_sem, all_send, all_sem,
):
    row, col = lax.axis_index("row"), lax.axis_index("col")
    R, C, h = row // 2, col, row % 2
    g = 1 - h
    diag, off = R == C, R != C
    fetch = pltpu.make_async_copy(adj, plain, adj_sem)
    fetch.start()

    barrier = pltpu.get_barrier_semaphore()

    def hello(r, c):
        pl.semaphore_signal(barrier, inc=1, device_id={"row": r, "col": c})

    for i in range(1, 8):
        hello(row, (C + i) % 8)
        hello(2 * ((R + i) % 8) + h, C)
    hello(2 * R + g, C)

    place = R * 8 + C
    kind = look_up(KIND, place)
    codes_a, codes_b = look_up(SENDS_A, place), look_up(SENDS_B, place)
    lhs_is_own = diag | (kind == 1)
    rhs_is_own = kind == 0

    p = lax.broadcasted_iota(I32, (8, 128), 1)
    column = 32 * (p % 4) + 16 * (p // 4 % 2) + p // 8
    fetch.wait()

    @pl.loop(0, 5)
    def _(i):
        at = pl.ds(pl.multiple_of(i * 8, 8), 8)
        for k in range(5):
            lanes = slice(k * 128, (k + 1) * 128)
            own[at, lanes] = jnp.take_along_axis(plain[at, lanes], column, axis=1)


    @pl.when(lhs_is_own)
    def _():
        inbox[7 + h] = own[...]

    @pl.when(rhs_is_own)
    def _():
        inbox[2] = own[...]

    pl.semaphore_wait(barrier, 15)

    def copy(src, dst, ssem, rsem, r, c):
        return pltpu.make_async_remote_copy(
            src_ref=src, dst_ref=dst, send_sem=ssem, recv_sem=rsem,
            device_id={"row": r, "col": c},
        )

    def offer(i):
        code = (codes_a if i < 4 else codes_b) // (128 ** (i % 4)) % 128
        slot, to, down = code % 4, code // 4 % 8, code // 32 % 2
        box = jnp.where(down == 1, 3 + 2 * slot + h, slot)
        r = jnp.where(down == 1, 2 * to + h, row)
        c = jnp.where(down == 1, col, to)
        return code >= 64, copy(own, inbox.at[box], send.at[i], in_sem.at[box], r, c)

    for i in range(7):
        there, c = offer(i)
        pl.when(there)(c.start)

    def relay(s):
        box = 3 + 2 * s + h
        return copy(inbox.at[box], inbox.at[box], relay_sem.at[s], in_sem.at[box], 2 * R + g, C)

    def arrived(box):
        copy(own, inbox.at[box], send.at[0], in_sem.at[box], row, col).wait_recv()

    def pass_on(s):
        @pl.when((s < 2) | jnp.logical_not(lhs_is_own))
        def _():
            arrived(3 + 2 * s + h)

        relay(s).start()

    first = jnp.where(diag, 2, 0)
    acc[...] = jnp.zeros_like(acc)
    pass_on(first)

    top = lax.broadcasted_iota(I32, (8, 128), 0) < 4
    upper = lax.broadcasted_iota(I32, (16, 128), 0) < 8
    bits = [
        jnp.where(upper, I32(1 << k), I32(1 << (k + 1) if k < 14 else -32768)).astype(jnp.int16)
        for k in range(0, 16, 2)
    ]

    def unpack(box, i, put):
        for k in range(5):
            words = inbox[box, pl.ds(pl.multiple_of(i * 8, 8), 8), k * 128 : (k + 1) * 128]
            for q in range(2):
                for j, piece in enumerate(unpacked(words[4 * q : 4 * q + 4], top, bits)):
                    put(q * 128 + j * 32, k * 128, piece)

    def product(lo, hi):
        for k in range(2):
            for i in range(lo, hi):
                def put(r, c, piece):
                    w_lhs[i * 256 + r : i * 256 + r + 32, k * ROWS + c : k * ROWS + c + 128] = piece
                unpack(3 + 2 * s_now[0] + k, i, put)
        at = slice(lo * 256, hi * 256)
        acc[at, :] += jnp.dot(w_lhs[at, :], w_rhs[...], preferred_element_type=F32)

    s_now = [None]

    @pl.loop(first, 3)
    def _(s):
        @pl.when((s < 2) | jnp.logical_not(rhs_is_own))
        def _():
            arrived(s)

        @pl.loop(0, 5)
        def _(i):
            def put(r, c, piece):
                w_rhs[pl.ds(pl.multiple_of(i * 256 + r, 32), 32), c : c + 128] = piece
            unpack(s, i, put)

        arrived(3 + 2 * s + g)
        s_now[0] = s
        product(0, 3)

        @pl.when(s < 2)
        def _():
            pass_on(s + 1)

        product(3, 5)

    def fold(i, closed):
        words = own[pl.ds(pl.multiple_of(i * 8, 8), 8), :]
        for q in range(2):
            part = halves(words[4 * q : 4 * q + 4], wide_top)
            sums = []
            for k in range(16):
                at = pl.multiple_of(i * 256 + q * 128 + k * 8, 8)
                val = jnp.where((part & (1 << k)) != 0, acc[pl.ds(at, 8), :], 0.0)
                closed = closed + val
                sums.append(sum(val[:, k * 128 : (k + 1) * 128] for k in range(5)))
            across = jnp.concatenate(sums, axis=0).T
            part_col[2 * i + q, :, :] = jnp.sum(across, axis=0, keepdims=True)
        return closed

    wide_top = lax.broadcasted_iota(I32, (8, ROWS), 0) < 4
    degree = jnp.sum(lax.population_count(own[...]), axis=0, keepdims=True).astype(F32)
    closed = lax.fori_loop(0, 5, fold, jnp.zeros((8, ROWS), F32))
    once_more = kind.astype(F32)
    closed = jnp.sum(closed, axis=0, keepdims=True) * (1.0 + once_more)
    part_col[...] = part_col[...] * (2.0 - once_more)
    for k in range(5):
        part_row[k, :, :] = closed[:, k * 128 : (k + 1) * 128]
        part_row[5 + k, :, :] = degree[:, k * 128 : (k + 1) * 128]

    give_row = [
        copy(part_row, red_row.at[C, h], send.at[7 + k], row_sem.at[C, h], 2 * R + k, R)
        for k in range(2)
    ]
    give_col = [
        copy(part_col, red_col.at[R, h], send.at[9 + k], col_sem.at[R, h], 2 * C + k, C)
        for k in range(2)
    ]

    @pl.when(off)
    def _():
        for c in give_row + give_col:
            c.start()

    to_other = copy(part_row, red_row.at[C, h], send.at[7], row_sem.at[C, h], 2 * R + g, C)
    pl.when(diag)(to_other.start)

    def tell(r, c):
        return copy(mine, every.at[R], all_send.at[r // 2 * 8 + c], all_sem.at[R], r, c)

    def for_all(act):
        for x in (0, 1, 3, 2):
            for y in (0, 1, 3, 2):
                @pl.loop(0, 4)
                def _(i):
                    r, c = y * 4 + x % 2 * 2 + h, x // 2 * 4 + i

                    @pl.when((r != row) | (c != col))
                    def _():
                        act(tell(r, c))

    @pl.when(diag)
    def _():
        copy(part_row, red_row.at[C, g], send.at[0], row_sem.at[C, g], row, col).wait_recv()
        red_row[C, h] = part_row[...]
        flat = jnp.zeros((10, 1, 128), F32)

        def add(i, carry):
            closed, degree, across = carry
            o = (R + i) % 8
            for k in range(2):
                copy(
                    part_row, red_row.at[o, k], send.at[0], row_sem.at[o, k], row, col
                ).wait_recv()
                copy(
                    part_col, red_col.at[o, k], send.at[0], col_sem.at[o, k], row, col
                ).wait_recv()
                across = across + red_col[o, k]
            sums = [red_row[o, k] for k in range(2)]
            closed = closed + jnp.concatenate([v[:5] for v in sums], axis=0)
            degree = degree + jnp.concatenate([v[5:] for v in sums], axis=0)
            return closed, degree, across

        sums = [red_row[C, k] for k in range(2)]
        closed = jnp.concatenate([v[:5] for v in sums], axis=0)
        degree = jnp.concatenate([v[5:] for v in sums], axis=0)
        closed, degree, across = lax.fori_loop(1, 8, add, (closed, degree, flat))
        total, deg = (closed + across)[:, 0, :], degree[:, 0, :]
        wedges = jnp.maximum(deg * (deg - 1.0), 1.0)
        mine[0:10, :] = total / wedges
        low = lax.broadcasted_iota(I32, (1, 128), 1) < 64
        both = []
        for v in (total, wedges):
            v = jnp.sum(v, axis=0, keepdims=True)
            both.append(v + pltpu.roll(v, 64, 1))
        mine[10:11, :] = jnp.where(low, both[0], both[1])
        every[C] = mine[...]
        for_all(lambda c: c.start())

    want_ref[...] = jnp.zeros_like(want_ref)
    want_ref[:, 0:80] = rel[...]
    want = jnp.broadcast_to(want_ref[...], (11, 128))
    block, rest = want // WIDE, want % WIDE
    line, lane = rest // 128, rest % 128
    lane = 8 * (lane % 16) + 4 * (lane // 16 % 2) + lane // 32
    here = lax.broadcasted_iota(I32, (11, 128), 0) == line

    for i in range(7):
        there, c = offer(i)
        pl.when(there)(c.wait_send)

    @pl.loop(first, 3)
    def _(s):
        relay(s).wait_send()

    @pl.when(off)
    def _():
        for c in give_row + give_col:
            c.wait_send()

    pl.when(diag)(to_other.wait_send)

    found = jnp.zeros((11, 128), F32)
    sums = jnp.zeros((1, 128), F32)
    for b in range(8):
        @pl.when(off | (R != b))
        def _():
            copy(mine, every.at[b], all_send.at[0], all_sem.at[b], row, col).wait_recv()

        tile = every[b]
        sums = sums + tile[10:11, :]
        got = jnp.take_along_axis(tile, lane, axis=1)
        found = found + jnp.where(here & (block == b), got, 0.0)
    low = lax.broadcasted_iota(I32, (1, 128), 1) < 64
    top = jnp.sum(jnp.where(low, sums, 0.0), axis=1, keepdims=True)
    bottom = jnp.sum(jnp.where(low, 0.0, sums), axis=1, keepdims=True)
    ratio_out[...] = top / bottom
    out[...] = jnp.sum(found, axis=0, keepdims=True)[:, 0:80]

    @pl.when(diag)
    def _():
        for_all(lambda c: c.wait_send())


def body(adjacency, relabel):
    dma = pltpu.SemaphoreType.DMA
    vmem = pltpu.VMEM
    out, ratio = pl.pallas_call(
        kernel,
        out_shape=(jax.ShapeDtypeStruct((1, 80), F32), jax.ShapeDtypeStruct((1, 1), F32)),
        in_specs=[pl.BlockSpec(memory_space=pl.ANY), pl.BlockSpec(memory_space=vmem)],
        out_specs=[pl.BlockSpec(memory_space=vmem)] * 2,
        scratch_shapes=[
            vmem((WORDS, ROWS), I32),
            vmem((WORDS, ROWS), I32),
            vmem((9, WORDS, ROWS), I32),
            vmem((WIDE, ROWS), F8),
            vmem((WIDE, WIDE), F8),
            vmem((WIDE, ROWS), F32),
            vmem((10, 1, 128), F32),
            vmem((10, 1, 128), F32),
            vmem((8, 2, 10, 1, 128), F32),
            vmem((8, 2, 10, 1, 128), F32),
            vmem((11, 128), F32),
            vmem((8, 11, 128), F32),
            vmem((1, 128), I32),
            dma,
            dma((11,)),
            dma((3,)),
            dma((9,)),
            dma((8, 2)),
            dma((8, 2)),
            dma((64,)),
            dma((8,)),
        ],
        compiler_params=pltpu.CompilerParams(
            collective_id=0, has_side_effects=True, vmem_limit_bytes=67043328
        ),
    )(adjacency.T, relabel[None, :])
    return out[0], ratio[0, 0]


def solution(mesh):
    placed = (P("row", "col"), P(("row", "col")))
    return jax.shard_map(
        body, mesh=mesh, in_specs=placed, out_specs=(P(("row", "col")), P()), check_vma=False
    )
```

```python
import jax
import jax.numpy as jnp
from jax import lax
from jax.experimental import pallas as pl
from jax.experimental.pallas import tpu as pltpu
from jax.sharding import PartitionSpec as P

SENDS_A = (
    257605490, 171736168, 196289112, 247346300, 180321384, 187856101, 146221640, 163478224,
    180190828, 266059126, 239023736, 187834460, 196833529, 171867756, 154369748, 137766988,
    179511888, 263991412, 240696694, 196507744, 162998848, 146570968, 230520928, 170948321,
    255668848, 171057236, 188185188, 249151346, 137460444, 154544196, 179991281, 222067300,
    146504808, 155089645, 179511896, 196506816, 257603426, 137919592, 162998856, 213791852,
    163020529, 138051180, 188444868, 171057244, 146374252, 266057062, 205469288, 154544204,
    196289104, 179597512, 263813216, 138377445, 146221632, 230436964, 240694630, 162691168,
    171537612, 187834452, 146111733, 255359588, 222114400, 137766980, 154368612, 249149282,
)
SENDS_B = (
    1286998, 0, 0, 0, 0, 0, 0, 0,
    0, 1220946, 0, 0, 0, 0, 0, 0,
    0, 0, 1287006, 0, 0, 0, 0, 0,
    0, 0, 0, 1220954, 0, 0, 0, 0,
    0, 0, 0, 0, 1551174, 0, 0, 0,
    0, 0, 0, 0, 0, 1485122, 0, 0,
    0, 0, 0, 0, 0, 0, 1551182, 0,
    0, 0, 0, 0, 0, 0, 0, 1485130,
)
KIND = (
    0, 7, 2, 7, 3, 4, 0, 1,
    7, 0, 7, 0, 4, 3, 1, 0,
    2, 7, 0, 7, 0, 1, 3, 6,
    7, 0, 7, 0, 1, 0, 6, 3,
    3, 4, 0, 1, 0, 7, 0, 7,
    4, 3, 1, 0, 7, 0, 7, 2,
    0, 1, 3, 6, 0, 7, 0, 7,
    1, 0, 6, 3, 7, 2, 7, 0,
)

F8 = jnp.float8_e4m3fn
I32 = jnp.int32
F32 = jnp.float32
WORDS, ROWS, WIDE = 40, 640, 1280


def look_up(table, d):
    return sum(jnp.where(d == i, I32(v), I32(0)) for i, v in enumerate(table) if v)


def halves(words, top):
    twice = jnp.concatenate([words, words], axis=0)
    return jnp.where(top, twice & 0xFFFF, lax.shift_right_logical(twice, 16))


def unpacked(words, top, bits):
    part = halves(words, top)
    part = jnp.concatenate([part, part], axis=0).astype(jnp.int16)
    one, none = jnp.bfloat16(1), jnp.bfloat16(0)
    rows = [jnp.where((part & b) != 0, one, none) for b in bits]
    return [jnp.concatenate(rows[2 * j : 2 * j + 2], axis=0).astype(F8) for j in range(4)]


def kernel(
    adj, rel, out, ratio_out,
    plain, own, inbox, w_rhs, w_lhs, acc, part_row, part_col, red_row, red_col, mine, every, want_ref,
    adj_sem, send, relay_sem, in_sem, row_sem, col_sem, all_send, all_sem,
):
    row, col = lax.axis_index("row"), lax.axis_index("col")
    R, C, h = row // 2, col, row % 2
    g = 1 - h
    diag, off = R == C, R != C
    fetch = pltpu.make_async_copy(adj, plain, adj_sem)
    fetch.start()

    barrier = pltpu.get_barrier_semaphore()

    def hello(r, c):
        pl.semaphore_signal(barrier, inc=1, device_id={"row": r, "col": c})

    for i in range(1, 8):
        hello(row, (C + i) % 8)
        hello(2 * ((R + i) % 8) + h, C)
    hello(2 * R + g, C)

    place = R * 8 + C
    kinds = look_up(KIND, place)
    kind = kinds // 4
    codes_a, codes_b = look_up(SENDS_A, place), look_up(SENDS_B, place)
    lhs_is_own = diag | (kind == 1)
    rhs_is_own = kind == 0

    p = lax.broadcasted_iota(I32, (8, 128), 1)
    column = 32 * (p % 4) + 16 * (p // 4 % 2) + p // 8
    fetch.wait()

    @pl.loop(0, 5)
    def _(i):
        at = pl.ds(pl.multiple_of(i * 8, 8), 8)
        for k in range(5):
            lanes = slice(k * 128, (k + 1) * 128)
            own[at, lanes] = jnp.take_along_axis(plain[at, lanes], column, axis=1)


    @pl.when(lhs_is_own)
    def _():
        inbox[7 + h] = own[...]

    @pl.when(rhs_is_own)
    def _():
        inbox[2] = own[...]

    pl.semaphore_wait(barrier, 15)

    def copy(src, dst, ssem, rsem, r, c):
        return pltpu.make_async_remote_copy(
            src_ref=src, dst_ref=dst, send_sem=ssem, recv_sem=rsem,
            device_id={"row": r, "col": c},
        )

    def offer(i):
        code = (codes_a if i < 4 else codes_b) // (128 ** (i % 4)) % 128
        slot, to, down = code % 4, code // 4 % 8, code // 32 % 2
        box = jnp.where(down == 1, 3 + 2 * slot + h, slot)
        r = jnp.where(down == 1, 2 * to + h, row)
        c = jnp.where(down == 1, col, to)
        return code >= 64, copy(own, inbox.at[box], send.at[i], in_sem.at[box], r, c)

    for i in range(7):
        there, c = offer(i)
        pl.when(there)(c.start)

    def relay(s):
        box = 3 + 2 * s + h
        return copy(inbox.at[box], inbox.at[box], relay_sem.at[s], in_sem.at[box], 2 * R + g, C)

    def arrived(box):
        copy(own, inbox.at[box], send.at[0], in_sem.at[box], row, col).wait_recv()

    def pass_on(s):
        @pl.when((s < 2) | jnp.logical_not(lhs_is_own))
        def _():
            arrived(3 + 2 * s + h)

        relay(s).start()

    first = jnp.where(diag, 2, 0)
    for k in range(2):
        acc[k] = jnp.zeros_like(acc[k])
    pass_on(first)

    top = lax.broadcasted_iota(I32, (8, 128), 0) < 4
    upper = lax.broadcasted_iota(I32, (16, 128), 0) < 8
    bits = [
        jnp.where(upper, I32(1 << k), I32(1 << (k + 1) if k < 14 else -32768)).astype(jnp.int16)
        for k in range(0, 16, 2)
    ]

    def unpack(box, i, put):
        for k in range(5):
            words = inbox[box, pl.ds(pl.multiple_of(i * 8, 8), 8), k * 128 : (k + 1) * 128]
            for q in range(2):
                for j, piece in enumerate(unpacked(words[4 * q : 4 * q + 4], top, bits)):
                    put(q * 128 + j * 32, k * 128, piece)

    def product(lo, hi):
        for k in range(2):
            for i in range(lo, hi):
                def put(r, c, piece):
                    w_lhs[i * 256 + r : i * 256 + r + 32, k * ROWS + c : k * ROWS + c + 128] = piece
                unpack(3 + 2 * s_now[0] + k, i, put)
        at = slice(lo * 256, hi * 256)
        acc[t_now[0], at, :] += jnp.dot(w_lhs[at, :], w_rhs[...], preferred_element_type=F32)

    s_now, t_now = [None], [None]

    @pl.loop(first, 3)
    def _(s):
        @pl.when((s < 2) | jnp.logical_not(rhs_is_own))
        def _():
            arrived(s)

        @pl.loop(0, 5)
        def _(i):
            def put(r, c, piece):
                w_rhs[pl.ds(pl.multiple_of(i * 256 + r, 32), 32), c : c + 128] = piece
            unpack(s, i, put)

        arrived(3 + 2 * s + g)
        s_now[0] = s
        t_now[0] = jnp.where(s == 0, kinds % 2, jnp.where(s == 1, kinds // 2 % 2, kind))
        product(0, 3)

        @pl.when(s < 2)
        def _():
            pass_on(s + 1)

        product(3, 5)

    def fold(i, closed):
        words = own[pl.ds(pl.multiple_of(i * 8, 8), 8), :]
        once, twice = closed
        for q in range(2):
            part = halves(words[4 * q : 4 * q + 4], wide_top)
            sums = []
            for k in range(16):
                at = pl.ds(pl.multiple_of(i * 256 + q * 128 + k * 8, 8), 8)
                bit = (part & (1 << k)) != 0
                a = jnp.where(bit, acc[0, at, :], 0.0)
                b = jnp.where(bit, acc[1, at, :], 0.0)
                once, twice = once + a, twice + b
                a = sum(a[:, k * 128 : (k + 1) * 128] for k in range(5))
                b = sum(b[:, k * 128 : (k + 1) * 128] for k in range(5))
                sums.append(2.0 * a + b)
            across = jnp.concatenate(sums, axis=0).T
            part_col[2 * i + q, :, :] = jnp.sum(across, axis=0, keepdims=True)
        return once, twice

    wide_top = lax.broadcasted_iota(I32, (8, ROWS), 0) < 4
    degree = jnp.sum(lax.population_count(own[...]), axis=0, keepdims=True).astype(F32)
    zeros = jnp.zeros((8, ROWS), F32)
    once, twice = lax.fori_loop(0, 5, fold, (zeros, zeros))
    closed = jnp.sum(once + 2.0 * twice, axis=0, keepdims=True)
    for k in range(5):
        part_row[k, :, :] = closed[:, k * 128 : (k + 1) * 128]
        part_row[5 + k, :, :] = degree[:, k * 128 : (k + 1) * 128]

    give_row = [
        copy(part_row, red_row.at[C, h], send.at[7 + k], row_sem.at[C, h], 2 * R + k, R)
        for k in range(2)
    ]
    give_col = [
        copy(part_col, red_col.at[R, h], send.at[9 + k], col_sem.at[R, h], 2 * C + k, C)
        for k in range(2)
    ]

    @pl.when(off)
    def _():
        for c in give_row + give_col:
            c.start()

    to_other = copy(part_row, red_row.at[C, h], send.at[7], row_sem.at[C, h], 2 * R + g, C)
    pl.when(diag)(to_other.start)

    def tell(r, c):
        return copy(mine, every.at[R], all_send.at[r // 2 * 8 + c], all_sem.at[R], r, c)

    def for_all(act):
        where = [(x, y, z) for x in range(4) for y in range(4) for z in range(4)]
        where.sort(key=lambda v: sum(min(a, 4 - a) for a in v))
        for x, y, z in where:
            r, c = y * 4 + x % 2 * 2 + h, x // 2 * 4 + z

            @pl.when((r != row) | (c != col))
            def _():
                act(tell(r, c))

    @pl.when(diag)
    def _():
        copy(part_row, red_row.at[C, g], send.at[0], row_sem.at[C, g], row, col).wait_recv()
        red_row[C, h] = part_row[...]
        flat = jnp.zeros((10, 1, 128), F32)

        def add(i, carry):
            closed, degree, across = carry
            o = (R + i) % 8
            for k in range(2):
                copy(
                    part_row, red_row.at[o, k], send.at[0], row_sem.at[o, k], row, col
                ).wait_recv()
                copy(
                    part_col, red_col.at[o, k], send.at[0], col_sem.at[o, k], row, col
                ).wait_recv()
                across = across + red_col[o, k]
            sums = [red_row[o, k] for k in range(2)]
            closed = closed + jnp.concatenate([v[:5] for v in sums], axis=0)
            degree = degree + jnp.concatenate([v[5:] for v in sums], axis=0)
            return closed, degree, across

        sums = [red_row[C, k] for k in range(2)]
        closed = jnp.concatenate([v[:5] for v in sums], axis=0)
        degree = jnp.concatenate([v[5:] for v in sums], axis=0)
        closed, degree, across = lax.fori_loop(1, 8, add, (closed, degree, flat))
        total, deg = (closed + across)[:, 0, :], degree[:, 0, :]
        wedges = jnp.maximum(deg * (deg - 1.0), 1.0)
        mine[0:10, :] = total / wedges
        low = lax.broadcasted_iota(I32, (1, 128), 1) < 64
        both = []
        for v in (total, wedges):
            v = jnp.sum(v, axis=0, keepdims=True)
            both.append(v + pltpu.roll(v, 64, 1))
        mine[10:11, :] = jnp.where(low, both[0], both[1])
        every[C] = mine[...]
        for_all(lambda c: c.start())

    want_ref[...] = jnp.zeros_like(want_ref)
    want_ref[:, 0:80] = rel[...]
    want = jnp.broadcast_to(want_ref[...], (11, 128))
    block, rest = want // WIDE, want % WIDE
    line, lane = rest // 128, rest % 128
    lane = 8 * (lane % 16) + 4 * (lane // 16 % 2) + lane // 32
    here = lax.broadcasted_iota(I32, (11, 128), 0) == line

    for i in range(7):
        there, c = offer(i)
        pl.when(there)(c.wait_send)

    @pl.loop(first, 3)
    def _(s):
        relay(s).wait_send()

    @pl.when(off)
    def _():
        for c in give_row + give_col:
            c.wait_send()

    pl.when(diag)(to_other.wait_send)

    found = jnp.zeros((11, 128), F32)
    sums = jnp.zeros((1, 128), F32)
    for b in range(8):
        @pl.when(off | (R != b))
        def _():
            copy(mine, every.at[b], all_send.at[0], all_sem.at[b], row, col).wait_recv()

        tile = every[b]
        sums = sums + tile[10:11, :]
        got = jnp.take_along_axis(tile, lane, axis=1)
        found = found + jnp.where(here & (block == b), got, 0.0)
    low = lax.broadcasted_iota(I32, (1, 128), 1) < 64
    top = jnp.sum(jnp.where(low, sums, 0.0), axis=1, keepdims=True)
    bottom = jnp.sum(jnp.where(low, 0.0, sums), axis=1, keepdims=True)
    ratio_out[...] = top / bottom
    out[...] = jnp.sum(found, axis=0, keepdims=True)[:, 0:80]

    @pl.when(diag)
    def _():
        for_all(lambda c: c.wait_send())


def body(adjacency, relabel):
    dma = pltpu.SemaphoreType.DMA
    vmem = pltpu.VMEM
    out, ratio = pl.pallas_call(
        kernel,
        out_shape=(jax.ShapeDtypeStruct((1, 80), F32), jax.ShapeDtypeStruct((1, 1), F32)),
        in_specs=[pl.BlockSpec(memory_space=pl.ANY), pl.BlockSpec(memory_space=vmem)],
        out_specs=[pl.BlockSpec(memory_space=vmem)] * 2,
        scratch_shapes=[
            vmem((WORDS, ROWS), I32),
            vmem((WORDS, ROWS), I32),
            vmem((9, WORDS, ROWS), I32),
            vmem((WIDE, ROWS), F8),
            vmem((WIDE, WIDE), F8),
            vmem((2, WIDE, ROWS), F32),
            vmem((10, 1, 128), F32),
            vmem((10, 1, 128), F32),
            vmem((8, 2, 10, 1, 128), F32),
            vmem((8, 2, 10, 1, 128), F32),
            vmem((11, 128), F32),
            vmem((8, 11, 128), F32),
            vmem((1, 128), I32),
            dma,
            dma((11,)),
            dma((3,)),
            dma((9,)),
            dma((8, 2)),
            dma((8, 2)),
            dma((64,)),
            dma((8,)),
        ],
        compiler_params=pltpu.CompilerParams(
            collective_id=0, has_side_effects=True, vmem_limit_bytes=67043328
        ),
    )(adjacency.T, relabel[None, :])
    return out[0], ratio[0, 0]


def solution(mesh):
    placed = (P("row", "col"), P(("row", "col")))
    return jax.shard_map(
        body, mesh=mesh, in_specs=placed, out_specs=(P(("row", "col")), P()), check_vma=False
    )
```

```python
import jax
import jax.numpy as jnp
from jax import lax
from jax.experimental import pallas as pl
from jax.experimental.pallas import tpu as pltpu
from jax.sharding import PartitionSpec as P

SENDS_A = (
    257605490, 171736168, 196289112, 247346300, 180321384, 187856101, 146221640, 163478224,
    180190828, 266059126, 239023736, 187834460, 196833529, 171867756, 154369748, 137766988,
    179511888, 263991412, 240696694, 196507744, 162998848, 146570968, 230520928, 170948321,
    255668848, 171057236, 188185188, 249151346, 137460444, 154544196, 179991281, 222067300,
    146504808, 155089645, 179511896, 196506816, 257603426, 137919592, 162998856, 213791852,
    163020529, 138051180, 188444868, 171057244, 146374252, 266057062, 205469288, 154544204,
    196289104, 179597512, 263813216, 138377445, 146221632, 230436964, 240694630, 162691168,
    171537612, 187834452, 146111733, 255359588, 222114400, 137766980, 154368612, 249149282,
)
SENDS_B = (
    1286998, 0, 0, 0, 0, 0, 0, 0,
    0, 1220946, 0, 0, 0, 0, 0, 0,
    0, 0, 1287006, 0, 0, 0, 0, 0,
    0, 0, 0, 1220954, 0, 0, 0, 0,
    0, 0, 0, 0, 1551174, 0, 0, 0,
    0, 0, 0, 0, 0, 1485122, 0, 0,
    0, 0, 0, 0, 0, 0, 1551182, 0,
    0, 0, 0, 0, 0, 0, 0, 1485130,
)
KIND = (
    0, 7, 2, 7, 3, 4, 0, 1,
    7, 0, 7, 0, 4, 3, 1, 0,
    2, 7, 0, 7, 0, 1, 3, 6,
    7, 0, 7, 0, 1, 0, 6, 3,
    3, 4, 0, 1, 0, 7, 0, 7,
    4, 3, 1, 0, 7, 0, 7, 2,
    0, 1, 3, 6, 0, 7, 0, 7,
    1, 0, 6, 3, 7, 2, 7, 0,
)

F8 = jnp.float8_e4m3fn
I32 = jnp.int32
F32 = jnp.float32
WORDS, ROWS, WIDE = 40, 640, 1280


def look_up(table, d):
    return sum(jnp.where(d == i, I32(v), I32(0)) for i, v in enumerate(table) if v)


def halves(words, top):
    twice = jnp.concatenate([words, words], axis=0)
    return jnp.where(top, twice & 0xFFFF, lax.shift_right_logical(twice, 16))


def unpacked(words, top, bits):
    part = halves(words, top)
    part = jnp.concatenate([part, part], axis=0).astype(jnp.int16)
    one, none = jnp.bfloat16(1), jnp.bfloat16(0)
    rows = [jnp.where((part & b) != 0, one, none) for b in bits]
    return [jnp.concatenate(rows[2 * j : 2 * j + 2], axis=0).astype(F8) for j in range(4)]


def kernel(
    adj, rel, out, ratio_out,
    plain, own, inbox, w_rhs, w_lhs, acc, part_row, part_col, red_row, red_col, mine, every, rel_here, want_ref,
    adj_sem, rel_sem, send, relay_sem, in_sem, row_sem, col_sem, all_send, all_sem,
):
    row, col = lax.axis_index("row"), lax.axis_index("col")
    R, C, h = row // 2, col, row % 2
    g = 1 - h
    diag, off = R == C, R != C
    fetch = pltpu.make_async_copy(adj, plain, adj_sem)
    fetch.start()
    fetch_rel = pltpu.make_async_copy(rel, rel_here, rel_sem)
    fetch_rel.start()

    barrier = pltpu.get_barrier_semaphore()

    def hello(r, c):
        pl.semaphore_signal(barrier, inc=1, device_id={"row": r, "col": c})

    for i in range(1, 8):
        hello(row, (C + i) % 8)
        hello(2 * ((R + i) % 8) + h, C)
    hello(2 * R + g, C)

    place = R * 8 + C
    kinds = look_up(KIND, place)
    kind = kinds // 4
    codes_a, codes_b = look_up(SENDS_A, place), look_up(SENDS_B, place)
    lhs_is_own = diag | (kind == 1)
    rhs_is_own = kind == 0

    p = lax.broadcasted_iota(I32, (8, 128), 1)
    column = 32 * (p % 4) + 16 * (p // 4 % 2) + p // 8
    fetch.wait()

    @pl.loop(0, 5)
    def _(i):
        at = pl.ds(pl.multiple_of(i * 8, 8), 8)
        for k in range(5):
            lanes = slice(k * 128, (k + 1) * 128)
            own[at, lanes] = jnp.take_along_axis(plain[at, lanes], column, axis=1)


    @pl.when(lhs_is_own)
    def _():
        inbox[7 + h] = own[...]

    @pl.when(rhs_is_own)
    def _():
        inbox[2] = own[...]

    pl.semaphore_wait(barrier, 15)

    def copy(src, dst, ssem, rsem, r, c):
        return pltpu.make_async_remote_copy(
            src_ref=src, dst_ref=dst, send_sem=ssem, recv_sem=rsem,
            device_id={"row": r, "col": c},
        )

    def offer(i):
        code = (codes_a if i < 4 else codes_b) // (128 ** (i % 4)) % 128
        slot, to, down = code % 4, code // 4 % 8, code // 32 % 2
        box = jnp.where(down == 1, 3 + 2 * slot + h, slot)
        r = jnp.where(down == 1, 2 * to + h, row)
        c = jnp.where(down == 1, col, to)
        return code >= 64, copy(own, inbox.at[box], send.at[i], in_sem.at[box], r, c)

    for i in range(7):
        there, c = offer(i)
        pl.when(there)(c.start)

    def relay(s):
        box = 3 + 2 * s + h
        return copy(inbox.at[box], inbox.at[box], relay_sem.at[s], in_sem.at[box], 2 * R + g, C)

    def arrived(box):
        copy(own, inbox.at[box], send.at[0], in_sem.at[box], row, col).wait_recv()

    def pass_on(s):
        @pl.when((s < 2) | jnp.logical_not(lhs_is_own))
        def _():
            arrived(3 + 2 * s + h)

        relay(s).start()

    first = jnp.where(diag, 2, 0)
    for k in range(2):
        acc[k] = jnp.zeros_like(acc[k])
    pass_on(first)

    top = lax.broadcasted_iota(I32, (8, 128), 0) < 4
    upper = lax.broadcasted_iota(I32, (16, 128), 0) < 8
    bits = [
        jnp.where(upper, I32(1 << k), I32(1 << (k + 1) if k < 14 else -32768)).astype(jnp.int16)
        for k in range(0, 16, 2)
    ]

    def unpack(box, i, put):
        for k in range(5):
            words = inbox[box, pl.ds(pl.multiple_of(i * 8, 8), 8), k * 128 : (k + 1) * 128]
            for q in range(2):
                for j, piece in enumerate(unpacked(words[4 * q : 4 * q + 4], top, bits)):
                    put(q * 128 + j * 32, k * 128, piece)

    def product(lo, hi):
        for k in range(2):
            for i in range(lo, hi):
                def put(r, c, piece):
                    w_lhs[i * 256 + r : i * 256 + r + 32, k * ROWS + c : k * ROWS + c + 128] = piece
                unpack(3 + 2 * s_now[0] + k, i, put)
        at = slice(lo * 256, hi * 256)
        acc[t_now[0], at, :] += jnp.dot(w_lhs[at, :], w_rhs[...], preferred_element_type=F32)

    s_now, t_now = [None], [None]

    @pl.loop(first, 3)
    def _(s):
        @pl.when((s < 2) | jnp.logical_not(rhs_is_own))
        def _():
            arrived(s)

        @pl.loop(0, 5)
        def _(i):
            def put(r, c, piece):
                w_rhs[pl.ds(pl.multiple_of(i * 256 + r, 32), 32), c : c + 128] = piece
            unpack(s, i, put)

        arrived(3 + 2 * s + g)
        s_now[0] = s
        t_now[0] = jnp.where(s == 0, kinds % 2, jnp.where(s == 1, kinds // 2 % 2, kind))
        product(0, 3)

        @pl.when(s < 2)
        def _():
            pass_on(s + 1)

        product(3, 5)

    def fold(i, closed):
        words = own[pl.ds(pl.multiple_of(i * 8, 8), 8), :]
        once, twice = closed
        for q in range(2):
            part = halves(words[4 * q : 4 * q + 4], wide_top)
            sums = []
            for k in range(16):
                at = pl.ds(pl.multiple_of(i * 256 + q * 128 + k * 8, 8), 8)
                bit = (part & (1 << k)) != 0
                a = jnp.where(bit, acc[0, at, :], 0.0)
                b = jnp.where(bit, acc[1, at, :], 0.0)
                once, twice = once + a, twice + b
                a = sum(a[:, k * 128 : (k + 1) * 128] for k in range(5))
                b = sum(b[:, k * 128 : (k + 1) * 128] for k in range(5))
                sums.append(2.0 * a + b)
            across = jnp.concatenate(sums, axis=0).T
            part_col[2 * i + q, :, :] = jnp.sum(across, axis=0, keepdims=True)
        return once, twice

    wide_top = lax.broadcasted_iota(I32, (8, ROWS), 0) < 4
    degree = jnp.sum(lax.population_count(own[...]), axis=0, keepdims=True).astype(F32)
    zeros = jnp.zeros((8, ROWS), F32)
    once, twice = lax.fori_loop(0, 5, fold, (zeros, zeros))
    closed = jnp.sum(once + 2.0 * twice, axis=0, keepdims=True)
    for k in range(5):
        part_row[k, :, :] = closed[:, k * 128 : (k + 1) * 128]
        part_row[5 + k, :, :] = degree[:, k * 128 : (k + 1) * 128]

    give_row = [
        copy(part_row, red_row.at[C, h], send.at[7 + k], row_sem.at[C, h], 2 * R + k, R)
        for k in range(2)
    ]
    give_col = [
        copy(part_col, red_col.at[R, h], send.at[9 + k], col_sem.at[R, h], 2 * C + k, C)
        for k in range(2)
    ]

    @pl.when(off)
    def _():
        for c in give_row + give_col:
            c.start()

    to_other = copy(part_row, red_row.at[C, h], send.at[7], row_sem.at[C, h], 2 * R + g, C)
    pl.when(diag)(to_other.start)

    def tell(r, c):
        return copy(mine, every.at[R], all_send.at[r // 2 * 8 + c], all_sem.at[R], r, c)

    def for_all(act):
        where = [(x, y, z) for x in range(4) for y in range(4) for z in range(4)]
        where.sort(key=lambda v: sum(min(a, 4 - a) for a in v))
        for x, y, z in where:
            r, c = y * 4 + x % 2 * 2 + h, x // 2 * 4 + z

            @pl.when((r != row) | (c != col))
            def _():
                act(tell(r, c))

    @pl.when(diag)
    def _():
        copy(part_row, red_row.at[C, g], send.at[0], row_sem.at[C, g], row, col).wait_recv()
        red_row[C, h] = part_row[...]
        flat = jnp.zeros((10, 1, 128), F32)

        def add(i, carry):
            closed, degree, across = carry
            o = (R + i) % 8
            for k in range(2):
                copy(
                    part_row, red_row.at[o, k], send.at[0], row_sem.at[o, k], row, col
                ).wait_recv()
                copy(
                    part_col, red_col.at[o, k], send.at[0], col_sem.at[o, k], row, col
                ).wait_recv()
                across = across + red_col[o, k]
            sums = [red_row[o, k] for k in range(2)]
            closed = closed + jnp.concatenate([v[:5] for v in sums], axis=0)
            degree = degree + jnp.concatenate([v[5:] for v in sums], axis=0)
            return closed, degree, across

        sums = [red_row[C, k] for k in range(2)]
        closed = jnp.concatenate([v[:5] for v in sums], axis=0)
        degree = jnp.concatenate([v[5:] for v in sums], axis=0)
        closed, degree, across = lax.fori_loop(1, 8, add, (closed, degree, flat))
        total, deg = (closed + across)[:, 0, :], degree[:, 0, :]
        wedges = jnp.maximum(deg * (deg - 1.0), 1.0)
        mine[0:10, :] = total / wedges
        low = lax.broadcasted_iota(I32, (1, 128), 1) < 64
        both = []
        for v in (total, wedges):
            v = jnp.sum(v, axis=0, keepdims=True)
            both.append(v + pltpu.roll(v, 64, 1))
        mine[10:11, :] = jnp.where(low, both[0], both[1])
        every[C] = mine[...]
        for_all(lambda c: c.start())

    want_ref[...] = jnp.zeros_like(want_ref)
    fetch_rel.wait()
    want_ref[:, 0:80] = rel_here[...]
    want = jnp.broadcast_to(want_ref[...], (11, 128))
    block, rest = want // WIDE, want % WIDE
    line, lane = rest // 128, rest % 128
    lane = 8 * (lane % 16) + 4 * (lane // 16 % 2) + lane // 32
    here = lax.broadcasted_iota(I32, (11, 128), 0) == line

    for i in range(7):
        there, c = offer(i)
        pl.when(there)(c.wait_send)

    @pl.loop(first, 3)
    def _(s):
        relay(s).wait_send()

    @pl.when(off)
    def _():
        for c in give_row + give_col:
            c.wait_send()

    pl.when(diag)(to_other.wait_send)

    found = jnp.zeros((11, 128), F32)
    sums = jnp.zeros((1, 128), F32)
    for b in range(8):
        @pl.when(off | (R != b))
        def _():
            copy(mine, every.at[b], all_send.at[0], all_sem.at[b], row, col).wait_recv()

        tile = every[b]
        sums = sums + tile[10:11, :]
        got = jnp.take_along_axis(tile, lane, axis=1)
        found = found + jnp.where(here & (block == b), got, 0.0)
    low = lax.broadcasted_iota(I32, (1, 128), 1) < 64
    top = jnp.sum(jnp.where(low, sums, 0.0), axis=1, keepdims=True)
    bottom = jnp.sum(jnp.where(low, 0.0, sums), axis=1, keepdims=True)
    ratio_out[...] = top / bottom
    out[...] = jnp.sum(found, axis=0, keepdims=True)[:, 0:80]

    @pl.when(diag)
    def _():
        for_all(lambda c: c.wait_send())


def body(adjacency, relabel):
    dma = pltpu.SemaphoreType.DMA
    vmem = pltpu.VMEM
    out, ratio = pl.pallas_call(
        kernel,
        out_shape=(jax.ShapeDtypeStruct((1, 80), F32), jax.ShapeDtypeStruct((1, 1), F32)),
        in_specs=[pl.BlockSpec(memory_space=pl.ANY)] * 2,
        out_specs=[pl.BlockSpec(memory_space=vmem)] * 2,
        scratch_shapes=[
            vmem((WORDS, ROWS), I32),
            vmem((WORDS, ROWS), I32),
            vmem((9, WORDS, ROWS), I32),
            vmem((WIDE, ROWS), F8),
            vmem((WIDE, WIDE), F8),
            vmem((2, WIDE, ROWS), F32),
            vmem((10, 1, 128), F32),
            vmem((10, 1, 128), F32),
            vmem((8, 2, 10, 1, 128), F32),
            vmem((8, 2, 10, 1, 128), F32),
            vmem((11, 128), F32),
            vmem((8, 11, 128), F32),
            vmem((1, 80), I32),
            vmem((1, 128), I32),
            dma,
            dma,
            dma((11,)),
            dma((3,)),
            dma((9,)),
            dma((8, 2)),
            dma((8, 2)),
            dma((64,)),
            dma((8,)),
        ],
        compiler_params=pltpu.CompilerParams(
            collective_id=0, has_side_effects=True, vmem_limit_bytes=67043328
        ),
    )(adjacency.T, relabel[None, :])
    return out[0], ratio[0, 0]


def solution(mesh):
    placed = (P("row", "col"), P(("row", "col")))
    return jax.shard_map(
        body, mesh=mesh, in_specs=placed, out_specs=(P(("row", "col")), P()), check_vma=False
    )
```

```python
import jax
import jax.numpy as jnp
from jax import lax
from jax.experimental import pallas as pl
from jax.experimental.pallas import tpu as pltpu
from jax.sharding import PartitionSpec as P

SENDS_A = (
    257605490, 171736168, 196289112, 247346300, 180321384, 187856101, 146221640, 163478224,
    180190828, 266059126, 239023736, 187834460, 196833529, 171867756, 154369748, 137766988,
    179511888, 263991412, 240696694, 196507744, 162998848, 146570968, 230520928, 170948321,
    255668848, 171057236, 188185188, 249151346, 137460444, 154544196, 179991281, 222067300,
    146504808, 155089645, 179511896, 196506816, 257603426, 137919592, 162998856, 213791852,
    163020529, 138051180, 188444868, 171057244, 146374252, 266057062, 205469288, 154544204,
    196289104, 179597512, 263813216, 138377445, 146221632, 230436964, 240694630, 162691168,
    171537612, 187834452, 146111733, 255359588, 222114400, 137766980, 154368612, 249149282,
)
SENDS_B = (
    1286998, 0, 0, 0, 0, 0, 0, 0,
    0, 1220946, 0, 0, 0, 0, 0, 0,
    0, 0, 1287006, 0, 0, 0, 0, 0,
    0, 0, 0, 1220954, 0, 0, 0, 0,
    0, 0, 0, 0, 1551174, 0, 0, 0,
    0, 0, 0, 0, 0, 1485122, 0, 0,
    0, 0, 0, 0, 0, 0, 1551182, 0,
    0, 0, 0, 0, 0, 0, 0, 1485130,
)
KIND = (
    0, 7, 2, 7, 3, 4, 0, 1,
    7, 0, 7, 0, 4, 3, 1, 0,
    2, 7, 0, 7, 0, 1, 3, 6,
    7, 0, 7, 0, 1, 0, 6, 3,
    3, 4, 0, 1, 0, 7, 0, 7,
    4, 3, 1, 0, 7, 0, 7, 2,
    0, 1, 3, 6, 0, 7, 0, 7,
    1, 0, 6, 3, 7, 2, 7, 0,
)

F8 = jnp.float8_e4m3fn
I32 = jnp.int32
F32 = jnp.float32
WORDS, ROWS, WIDE = 40, 640, 1280


def look_up(table, d):
    return sum(jnp.where(d == i, I32(v), I32(0)) for i, v in enumerate(table) if v)


def halves(words, top):
    twice = jnp.concatenate([words, words], axis=0)
    return jnp.where(top, twice & 0xFFFF, lax.shift_right_logical(twice, 16))


def unpacked(words, top, bits):
    part = halves(words, top)
    part = jnp.concatenate([part, part], axis=0).astype(jnp.int16)
    one, none = jnp.bfloat16(1), jnp.bfloat16(0)
    rows = [jnp.where((part & b) != 0, one, none) for b in bits]
    return [jnp.concatenate(rows[2 * j : 2 * j + 2], axis=0).astype(F8) for j in range(4)]


def kernel(
    adj, rel, out, ratio_out,
    plain, own, inbox, w_rhs, w_lhs, part_row, part_col, red_row, red_col, mine, every, rel_here, want_ref,
    adj_sem, rel_sem, send, relay_sem, in_sem, row_sem, col_sem, all_send, all_sem,
):
    row, col = lax.axis_index("row"), lax.axis_index("col")
    R, C, h = row // 2, col, row % 2
    g = 1 - h
    diag, off = R == C, R != C
    fetch = pltpu.make_async_copy(adj, plain, adj_sem)
    fetch.start()
    fetch_rel = pltpu.make_async_copy(rel, rel_here, rel_sem)
    fetch_rel.start()

    barrier = pltpu.get_barrier_semaphore()

    def hello(r, c):
        pl.semaphore_signal(barrier, inc=1, device_id={"row": r, "col": c})

    for i in range(1, 8):
        hello(row, (C + i) % 8)
        hello(2 * ((R + i) % 8) + h, C)
    hello(2 * R + g, C)

    place = R * 8 + C
    kinds = look_up(KIND, place)
    kind = kinds // 4
    codes_a, codes_b = look_up(SENDS_A, place), look_up(SENDS_B, place)
    lhs_is_own = diag | (kind == 1)
    rhs_is_own = kind == 0

    p = lax.broadcasted_iota(I32, (8, 128), 1)
    column = 32 * (p % 4) + 16 * (p // 4 % 2) + p // 8
    fetch.wait()

    @pl.loop(0, 5)
    def _(i):
        at = pl.ds(pl.multiple_of(i * 8, 8), 8)
        for k in range(5):
            lanes = slice(k * 128, (k + 1) * 128)
            own[at, lanes] = jnp.take_along_axis(plain[at, lanes], column, axis=1)


    @pl.when(lhs_is_own)
    def _():
        inbox[7 + h] = own[...]

    @pl.when(rhs_is_own)
    def _():
        inbox[2] = own[...]

    pl.semaphore_wait(barrier, 15)

    def copy(src, dst, ssem, rsem, r, c):
        return pltpu.make_async_remote_copy(
            src_ref=src, dst_ref=dst, send_sem=ssem, recv_sem=rsem,
            device_id={"row": r, "col": c},
        )

    def offer(i):
        code = (codes_a if i < 4 else codes_b) // (128 ** (i % 4)) % 128
        slot, to, down = code % 4, code // 4 % 8, code // 32 % 2
        box = jnp.where(down == 1, 3 + 2 * slot + h, slot)
        r = jnp.where(down == 1, 2 * to + h, row)
        c = jnp.where(down == 1, col, to)
        return code >= 64, copy(own, inbox.at[box], send.at[i], in_sem.at[box], r, c)

    for i in range(7):
        there, c = offer(i)
        pl.when(there)(c.start)

    def relay(s):
        box = 3 + 2 * s + h
        return copy(inbox.at[box], inbox.at[box], relay_sem.at[s], in_sem.at[box], 2 * R + g, C)

    def arrived(box):
        copy(own, inbox.at[box], send.at[0], in_sem.at[box], row, col).wait_recv()

    def pass_on(s):
        @pl.when((s < 2) | jnp.logical_not(lhs_is_own))
        def _():
            arrived(3 + 2 * s + h)

        relay(s).start()

    last = jnp.where(diag, 1, 3)
    degree = jnp.sum(lax.population_count(own[...]), axis=0, keepdims=True).astype(F32)
    part_row[...] = jnp.zeros_like(part_row)
    part_col[...] = jnp.zeros_like(part_col)
    for k in range(5):
        part_row[5 + k, :, :] = degree[:, k * 128 : (k + 1) * 128]
    pass_on(2)

    top = lax.broadcasted_iota(I32, (8, 128), 0) < 4
    upper = lax.broadcasted_iota(I32, (16, 128), 0) < 8
    bits = [
        jnp.where(upper, I32(1 << k), I32(1 << (k + 1) if k < 14 else -32768)).astype(jnp.int16)
        for k in range(0, 16, 2)
    ]

    def unpack(box, i, put):
        for k in range(5):
            words = inbox[box, pl.ds(pl.multiple_of(i * 8, 8), 8), k * 128 : (k + 1) * 128]
            for q in range(2):
                for j, piece in enumerate(unpacked(words[4 * q : 4 * q + 4], top, bits)):
                    put(q * 128 + j * 32, k * 128, piece)

    def product(lo, hi):
        for k in range(2):
            for i in range(lo, hi):
                def put(r, c, piece):
                    w_lhs[i * 256 + r : i * 256 + r + 32, k * ROWS + c : k * ROWS + c + 128] = piece
                unpack(3 + 2 * s_now[0] + k, i, put)
        at = slice(lo * 256, hi * 256)
        paths = jnp.dot(w_lhs[at, :], w_rhs[...], preferred_element_type=F32)
        closed = jnp.zeros((8, ROWS), F32)
        for n in range(2 * (hi - lo)):
            words = own[(2 * lo + n) * 4 : (2 * lo + n) * 4 + 4, :]
            part = halves(words, wide_top)
            sums = []
            for k in range(16):
                r = n * 128 + k * 8
                val = jnp.where((part & (1 << k)) != 0, paths[r : r + 8, :], 0.0)
                closed = closed + val
                sums.append(sum(val[:, j * 128 : (j + 1) * 128] for j in range(5)))
            across = jnp.sum(jnp.concatenate(sums, axis=0).T, axis=0, keepdims=True)
            part_col[2 * lo + n, :, :] += across * (2.0 - t_now[0])
        closed = jnp.sum(closed, axis=0, keepdims=True) * (1.0 + t_now[0])
        for k in range(5):
            part_row[k, :, :] += closed[:, k * 128 : (k + 1) * 128]

    wide_top = lax.broadcasted_iota(I32, (8, ROWS), 0) < 4
    s_now, t_now = [None], [None]

    @pl.loop(0, last)
    def _(turn):
        s = (turn + 2) % 3

        @pl.when((s < 2) | jnp.logical_not(rhs_is_own))
        def _():
            arrived(s)

        @pl.loop(0, 5)
        def _(i):
            def put(r, c, piece):
                w_rhs[pl.ds(pl.multiple_of(i * 256 + r, 32), 32), c : c + 128] = piece
            unpack(s, i, put)

        arrived(3 + 2 * s + g)

        @pl.when(turn + 1 < last)
        def _():
            pass_on(turn)

        s_now[0] = s
        t_now[0] = jnp.where(
            s == 0, kinds % 2, jnp.where(s == 1, kinds // 2 % 2, kind)
        ).astype(F32)
        product(0, 3)

        product(3, 5)

    give_row = [
        copy(part_row, red_row.at[C, h], send.at[7 + k], row_sem.at[C, h], 2 * R + k, R)
        for k in range(2)
    ]
    give_col = [
        copy(part_col, red_col.at[R, h], send.at[9 + k], col_sem.at[R, h], 2 * C + k, C)
        for k in range(2)
    ]

    @pl.when(off)
    def _():
        for c in give_row + give_col:
            c.start()

    to_other = copy(part_row, red_row.at[C, h], send.at[7], row_sem.at[C, h], 2 * R + g, C)
    pl.when(diag)(to_other.start)

    def tell(r, c):
        return copy(mine, every.at[R], all_send.at[r // 2 * 8 + c], all_sem.at[R], r, c)

    def for_all(act):
        where = [(x, y, z) for x in range(4) for y in range(4) for z in range(4)]
        where.sort(key=lambda v: sum(min(a, 4 - a) for a in v))
        for x, y, z in where:
            r, c = y * 4 + x % 2 * 2 + h, x // 2 * 4 + z

            @pl.when((r != row) | (c != col))
            def _():
                act(tell(r, c))

    @pl.when(diag)
    def _():
        copy(part_row, red_row.at[C, g], send.at[0], row_sem.at[C, g], row, col).wait_recv()
        red_row[C, h] = part_row[...]
        flat = jnp.zeros((10, 1, 128), F32)

        def add(i, carry):
            closed, degree, across = carry
            o = (R + i) % 8
            for k in range(2):
                copy(
                    part_row, red_row.at[o, k], send.at[0], row_sem.at[o, k], row, col
                ).wait_recv()
                copy(
                    part_col, red_col.at[o, k], send.at[0], col_sem.at[o, k], row, col
                ).wait_recv()
                across = across + red_col[o, k]
            sums = [red_row[o, k] for k in range(2)]
            closed = closed + jnp.concatenate([v[:5] for v in sums], axis=0)
            degree = degree + jnp.concatenate([v[5:] for v in sums], axis=0)
            return closed, degree, across

        sums = [red_row[C, k] for k in range(2)]
        closed = jnp.concatenate([v[:5] for v in sums], axis=0)
        degree = jnp.concatenate([v[5:] for v in sums], axis=0)
        closed, degree, across = lax.fori_loop(1, 8, add, (closed, degree, flat))
        total, deg = (closed + across)[:, 0, :], degree[:, 0, :]
        wedges = jnp.maximum(deg * (deg - 1.0), 1.0)
        mine[0:10, :] = total / wedges
        low = lax.broadcasted_iota(I32, (1, 128), 1) < 64
        both = []
        for v in (total, wedges):
            v = jnp.sum(v, axis=0, keepdims=True)
            both.append(v + pltpu.roll(v, 64, 1))
        mine[10:11, :] = jnp.where(low, both[0], both[1])
        every[C] = mine[...]
        for_all(lambda c: c.start())

    want_ref[...] = jnp.zeros_like(want_ref)
    fetch_rel.wait()
    want_ref[:, 0:80] = rel_here[...]
    want = jnp.broadcast_to(want_ref[...], (11, 128))
    block, rest = want // WIDE, want % WIDE
    line, lane = rest // 128, rest % 128
    lane = 8 * (lane % 16) + 4 * (lane // 16 % 2) + lane // 32
    here = lax.broadcasted_iota(I32, (11, 128), 0) == line

    for i in range(7):
        there, c = offer(i)
        pl.when(there)(c.wait_send)

    @pl.loop(0, last)
    def _(turn):
        relay((turn + 2) % 3).wait_send()

    @pl.when(off)
    def _():
        for c in give_row + give_col:
            c.wait_send()

    pl.when(diag)(to_other.wait_send)

    found = jnp.zeros((11, 128), F32)
    sums = jnp.zeros((1, 128), F32)
    for b in range(8):
        @pl.when(off | (R != b))
        def _():
            copy(mine, every.at[b], all_send.at[0], all_sem.at[b], row, col).wait_recv()

        tile = every[b]
        sums = sums + tile[10:11, :]
        got = jnp.take_along_axis(tile, lane, axis=1)
        found = found + jnp.where(here & (block == b), got, 0.0)
    low = lax.broadcasted_iota(I32, (1, 128), 1) < 64
    top = jnp.sum(jnp.where(low, sums, 0.0), axis=1, keepdims=True)
    bottom = jnp.sum(jnp.where(low, 0.0, sums), axis=1, keepdims=True)
    ratio_out[...] = top / bottom
    out[...] = jnp.sum(found, axis=0, keepdims=True)[:, 0:80]

    @pl.when(diag)
    def _():
        for_all(lambda c: c.wait_send())


def body(adjacency, relabel):
    dma = pltpu.SemaphoreType.DMA
    vmem = pltpu.VMEM
    out, ratio = pl.pallas_call(
        kernel,
        out_shape=(jax.ShapeDtypeStruct((1, 80), F32), jax.ShapeDtypeStruct((1, 1), F32)),
        in_specs=[pl.BlockSpec(memory_space=pl.ANY)] * 2,
        out_specs=[pl.BlockSpec(memory_space=vmem)] * 2,
        scratch_shapes=[
            vmem((WORDS, ROWS), I32),
            vmem((WORDS, ROWS), I32),
            vmem((9, WORDS, ROWS), I32),
            vmem((WIDE, ROWS), F8),
            vmem((WIDE, WIDE), F8),
            vmem((10, 1, 128), F32),
            vmem((10, 1, 128), F32),
            vmem((8, 2, 10, 1, 128), F32),
            vmem((8, 2, 10, 1, 128), F32),
            vmem((11, 128), F32),
            vmem((8, 11, 128), F32),
            vmem((1, 80), I32),
            vmem((1, 128), I32),
            dma,
            dma,
            dma((11,)),
            dma((3,)),
            dma((9,)),
            dma((8, 2)),
            dma((8, 2)),
            dma((64,)),
            dma((8,)),
        ],
        compiler_params=pltpu.CompilerParams(
            collective_id=0, has_side_effects=True, vmem_limit_bytes=67043328
        ),
    )(adjacency.T, relabel[None, :])
    return out[0], ratio[0, 0]


def solution(mesh):
    placed = (P("row", "col"), P(("row", "col")))
    return jax.shard_map(
        body, mesh=mesh, in_specs=placed, out_specs=(P(("row", "col")), P()), check_vma=False
    )
```

```python
import jax
import jax.numpy as jnp
from jax import lax
from jax.experimental import pallas as pl
from jax.experimental.pallas import tpu as pltpu
from jax.sharding import PartitionSpec as P

SENDS_A = (
    257605490, 171736168, 196289112, 247346300, 180321384, 187856101, 146221640, 163478224,
    180190828, 266059126, 239023736, 187834460, 196833529, 171867756, 154369748, 137766988,
    179511888, 263991412, 240696694, 196507744, 162998848, 146570968, 230520928, 170948321,
    255668848, 171057236, 188185188, 249151346, 137460444, 154544196, 179991281, 222067300,
    146504808, 155089645, 179511896, 196506816, 257603426, 137919592, 162998856, 213791852,
    163020529, 138051180, 188444868, 171057244, 146374252, 266057062, 205469288, 154544204,
    196289104, 179597512, 263813216, 138377445, 146221632, 230436964, 240694630, 162691168,
    171537612, 187834452, 146111733, 255359588, 222114400, 137766980, 154368612, 249149282,
)
SENDS_B = (
    1286998, 0, 0, 0, 0, 0, 0, 0,
    0, 1220946, 0, 0, 0, 0, 0, 0,
    0, 0, 1287006, 0, 0, 0, 0, 0,
    0, 0, 0, 1220954, 0, 0, 0, 0,
    0, 0, 0, 0, 1551174, 0, 0, 0,
    0, 0, 0, 0, 0, 1485122, 0, 0,
    0, 0, 0, 0, 0, 0, 1551182, 0,
    0, 0, 0, 0, 0, 0, 0, 1485130,
)
KIND = (
    0, 7, 2, 7, 3, 4, 0, 1,
    7, 0, 7, 0, 4, 3, 1, 0,
    2, 7, 0, 7, 0, 1, 3, 6,
    7, 0, 7, 0, 1, 0, 6, 3,
    3, 4, 0, 1, 0, 7, 0, 7,
    4, 3, 1, 0, 7, 0, 7, 2,
    0, 1, 3, 6, 0, 7, 0, 7,
    1, 0, 6, 3, 7, 2, 7, 0,
)

F8 = jnp.float8_e4m3fn
I32 = jnp.int32
F32 = jnp.float32
WORDS, ROWS, WIDE = 40, 640, 1280


def look_up(table, d):
    return sum(jnp.where(d == i, I32(v), I32(0)) for i, v in enumerate(table) if v)


def halves(words, top):
    twice = jnp.concatenate([words, words], axis=0)
    return jnp.where(top, twice & 0xFFFF, lax.shift_right_logical(twice, 16))


def unpacked(words, top, bits):
    part = halves(words, top)
    part = jnp.concatenate([part, part], axis=0).astype(jnp.int16)
    one, none = jnp.bfloat16(1), jnp.bfloat16(0)
    rows = [jnp.where((part & b) != 0, one, none) for b in bits]
    return [jnp.concatenate(rows[2 * j : 2 * j + 2], axis=0).astype(F8) for j in range(4)]


def kernel(
    adj, rel, out, ratio_out,
    plain, own, inbox, w_rhs, w_lhs, part_row, part_col, red_row, red_col, mine, every, rel_here, want_ref,
    adj_sem, rel_sem, send, relay_sem, in_sem, row_sem, col_sem, all_send, all_sem,
):
    row, col = lax.axis_index("row"), lax.axis_index("col")
    R, C, h = row // 2, col, row % 2
    g = 1 - h
    diag, off = R == C, R != C
    fetch = pltpu.make_async_copy(adj, plain, adj_sem)
    fetch.start()
    fetch_rel = pltpu.make_async_copy(rel, rel_here, rel_sem)
    fetch_rel.start()

    barrier = pltpu.get_barrier_semaphore()

    def hello(r, c):
        pl.semaphore_signal(barrier, inc=1, device_id={"row": r, "col": c})

    for i in range(1, 8):
        hello(row, (C + i) % 8)
        hello(2 * ((R + i) % 8) + h, C)
    hello(2 * R + g, C)

    place = R * 8 + C
    kinds = look_up(KIND, place)
    kind = kinds // 4
    codes_a, codes_b = look_up(SENDS_A, place), look_up(SENDS_B, place)
    lhs_is_own = diag | (kind == 1)
    rhs_is_own = kind == 0

    p = lax.broadcasted_iota(I32, (8, 128), 1)
    column = 32 * (p % 4) + 16 * (p // 4 % 2) + p // 8
    fetch.wait()

    @pl.loop(0, 5)
    def _(i):
        at = pl.ds(pl.multiple_of(i * 8, 8), 8)
        for k in range(5):
            lanes = slice(k * 128, (k + 1) * 128)
            own[at, lanes] = jnp.take_along_axis(plain[at, lanes], column, axis=1)


    @pl.when(lhs_is_own)
    def _():
        inbox[7 + h] = own[...]

    @pl.when(rhs_is_own)
    def _():
        inbox[2] = own[...]

    pl.semaphore_wait(barrier, 15)

    def copy(src, dst, ssem, rsem, r, c):
        return pltpu.make_async_remote_copy(
            src_ref=src, dst_ref=dst, send_sem=ssem, recv_sem=rsem,
            device_id={"row": r, "col": c},
        )

    def offer(i):
        code = (codes_a if i < 4 else codes_b) // (128 ** (i % 4)) % 128
        slot, to, down = code % 4, code // 4 % 8, code // 32 % 2
        box = jnp.where(down == 1, 3 + 2 * slot + h, slot)
        r = jnp.where(down == 1, 2 * to + h, row)
        c = jnp.where(down == 1, col, to)
        return code >= 64, copy(own, inbox.at[box], send.at[i], in_sem.at[box], r, c)

    for i in range(7):
        there, c = offer(i)
        pl.when(there)(c.start)

    def relay(s):
        box = 3 + 2 * s + h
        return copy(inbox.at[box], inbox.at[box], relay_sem.at[s], in_sem.at[box], 2 * R + g, C)

    def arrived(box):
        copy(own, inbox.at[box], send.at[0], in_sem.at[box], row, col).wait_recv()

    def pass_on(s):
        @pl.when((s < 2) | jnp.logical_not(lhs_is_own))
        def _():
            arrived(3 + 2 * s + h)

        relay(s).start()

    last = jnp.where(diag, 1, 3)
    degree = jnp.sum(lax.population_count(own[...]), axis=0, keepdims=True).astype(F32)
    part_row[...] = jnp.zeros_like(part_row)
    part_col[...] = jnp.zeros_like(part_col)
    for k in range(5):
        part_row[5 + k, :, :] = degree[:, k * 128 : (k + 1) * 128]
    pass_on(2)

    top = lax.broadcasted_iota(I32, (8, 128), 0) < 4
    upper = lax.broadcasted_iota(I32, (16, 128), 0) < 8
    bits = [
        jnp.where(upper, I32(1 << k), I32(1 << (k + 1) if k < 14 else -32768)).astype(jnp.int16)
        for k in range(0, 16, 2)
    ]

    def unpack(box, i, put):
        for k in range(5):
            words = inbox[box, pl.ds(pl.multiple_of(i * 8, 8), 8), k * 128 : (k + 1) * 128]
            for q in range(2):
                for j, piece in enumerate(unpacked(words[4 * q : 4 * q + 4], top, bits)):
                    put(q * 128 + j * 32, k * 128, piece)

    def product(lo, hi):
        for k in range(2):
            for i in range(lo, hi):
                def put(r, c, piece):
                    w_lhs[i * 256 + r : i * 256 + r + 32, k * ROWS + c : k * ROWS + c + 128] = piece
                unpack(3 + 2 * s_now[0] + k, i, put)
        at = slice(lo * 256, hi * 256)
        paths = jnp.dot(w_lhs[at, :], w_rhs[...], preferred_element_type=F32)
        closed = jnp.zeros((8, ROWS), F32)
        for n in range(2 * (hi - lo)):
            words = own[(2 * lo + n) * 4 : (2 * lo + n) * 4 + 4, :]
            part = halves(words, wide_top)
            sums = []
            for k in range(16):
                r = n * 128 + k * 8
                val = jnp.where((part & (1 << k)) != 0, paths[r : r + 8, :], 0.0)
                closed = closed + val
                sums.append(sum(val[:, j * 128 : (j + 1) * 128] for j in range(5)))
            across = jnp.sum(jnp.concatenate(sums, axis=0).T, axis=0, keepdims=True)
            part_col[2 * lo + n, :, :] += across * (2.0 - t_now[0])
        closed = jnp.sum(closed, axis=0, keepdims=True) * (1.0 + t_now[0])
        for k in range(5):
            part_row[k, :, :] += closed[:, k * 128 : (k + 1) * 128]

    wide_top = lax.broadcasted_iota(I32, (8, ROWS), 0) < 4
    s_now, t_now = [None], [None]

    @pl.loop(0, last)
    def _(turn):
        s = (turn + 2) % 3

        @pl.when((s < 2) | jnp.logical_not(rhs_is_own))
        def _():
            arrived(s)

        @pl.loop(0, 5)
        def _(i):
            def put(r, c, piece):
                w_rhs[pl.ds(pl.multiple_of(i * 256 + r, 32), 32), c : c + 128] = piece
            unpack(s, i, put)

        arrived(3 + 2 * s + g)

        @pl.when(turn + 1 < last)
        def _():
            pass_on(turn)

        s_now[0] = s
        t_now[0] = jnp.where(
            s == 0, kinds % 2, jnp.where(s == 1, kinds // 2 % 2, kind)
        ).astype(F32)
        product(0, 3)

        product(3, 5)

    give_row = [
        copy(part_row, red_row.at[C, h], send.at[7 + k], row_sem.at[C, h], 2 * R + k, R)
        for k in range(2)
    ]
    give_col = [
        copy(part_col, red_col.at[R, h], send.at[9 + k], col_sem.at[R, h], 2 * C + k, C)
        for k in range(2)
    ]

    @pl.when(off)
    def _():
        for c in give_row + give_col:
            c.start()

    to_other = copy(part_row, red_row.at[C, h], send.at[7], row_sem.at[C, h], 2 * R + g, C)
    pl.when(diag)(to_other.start)

    def tell(r, c):
        return copy(mine, every.at[R], all_send.at[r // 2 * 8 + c], all_sem.at[R], r, c)

    def for_all(act):
        where = [(x, y, z) for x in range(4) for y in range(4) for z in range(4)]
        where.sort(key=lambda v: sum(min(a, 4 - a) for a in v))
        for x, y, z in where:
            r, c = y * 4 + x % 2 * 2 + h, x // 2 * 4 + z

            @pl.when((r != row) | (c != col))
            def _():
                act(tell(r, c))

    @pl.when(diag)
    def _():
        copy(part_row, red_row.at[C, g], send.at[0], row_sem.at[C, g], row, col).wait_recv()
        red_row[C, h] = part_row[...]
        flat = jnp.zeros((10, 1, 128), F32)

        def add(i, carry):
            closed, degree, across = carry
            o = (R + i) % 8
            for k in range(2):
                copy(
                    part_row, red_row.at[o, k], send.at[0], row_sem.at[o, k], row, col
                ).wait_recv()
                copy(
                    part_col, red_col.at[o, k], send.at[0], col_sem.at[o, k], row, col
                ).wait_recv()
                across = across + red_col[o, k]
            sums = [red_row[o, k] for k in range(2)]
            closed = closed + jnp.concatenate([v[:5] for v in sums], axis=0)
            degree = degree + jnp.concatenate([v[5:] for v in sums], axis=0)
            return closed, degree, across

        sums = [red_row[C, k] for k in range(2)]
        closed = jnp.concatenate([v[:5] for v in sums], axis=0)
        degree = jnp.concatenate([v[5:] for v in sums], axis=0)
        closed, degree, across = lax.fori_loop(1, 8, add, (closed, degree, flat))
        total, deg = (closed + across)[:, 0, :], degree[:, 0, :]
        wedges = jnp.maximum(deg * (deg - 1.0), 1.0)
        mine[0:10, :] = total / wedges
        low = lax.broadcasted_iota(I32, (1, 128), 1) < 64
        both = []
        for v in (total, wedges):
            v = jnp.sum(v, axis=0, keepdims=True)
            both.append(v + pltpu.roll(v, 64, 1))
        mine[10:11, :] = jnp.where(low, both[0], both[1])
        every[C] = mine[...]
        for_all(lambda c: c.start())

    want_ref[...] = jnp.zeros_like(want_ref)
    fetch_rel.wait()
    want_ref[:, 0:80] = rel_here[...]
    want = jnp.broadcast_to(want_ref[...], (11, 128))
    block, rest = want // WIDE, want % WIDE
    line, lane = rest // 128, rest % 128
    lane = 8 * (lane % 16) + 4 * (lane // 16 % 2) + lane // 32
    here = lax.broadcasted_iota(I32, (11, 128), 0) == line

    for i in range(7):
        there, c = offer(i)
        pl.when(there)(c.wait_send)

    @pl.loop(0, last)
    def _(turn):
        relay((turn + 2) % 3).wait_send()

    @pl.when(off)
    def _():
        for c in give_row + give_col:
            c.wait_send()

    pl.when(diag)(to_other.wait_send)

    found = jnp.zeros((11, 128), F32)
    sums = jnp.zeros((1, 128), F32)
    for b in range(8):
        @pl.when(off | (R != b))
        def _():
            copy(mine, every.at[b], all_send.at[0], all_sem.at[b], row, col).wait_recv()

        tile = every[b]
        sums = sums + tile[10:11, :]
        got = jnp.take_along_axis(tile, lane, axis=1)
        found = found + jnp.where(here & (block == b), got, 0.0)
    low = lax.broadcasted_iota(I32, (1, 128), 1) < 64
    top = jnp.sum(jnp.where(low, sums, 0.0), axis=1, keepdims=True)
    bottom = jnp.sum(jnp.where(low, 0.0, sums), axis=1, keepdims=True)
    ratio_out[...] = top / bottom
    out[...] = jnp.sum(found, axis=0, keepdims=True)[:, 0:80]

    @pl.when(diag)
    def _():
        for_all(lambda c: c.wait_send())


def body(adjacency, relabel):
    dma = pltpu.SemaphoreType.DMA
    vmem = pltpu.VMEM
    out, ratio = pl.pallas_call(
        kernel,
        out_shape=(jax.ShapeDtypeStruct((1, 80), F32), jax.ShapeDtypeStruct((1, 1), F32)),
        in_specs=[pl.BlockSpec(memory_space=pl.ANY)] * 2,
        out_specs=[pl.BlockSpec(memory_space=vmem)] * 2,
        scratch_shapes=[
            vmem((WORDS, ROWS), I32),
            vmem((WORDS, ROWS), I32),
            vmem((9, WORDS, ROWS), I32),
            vmem((WIDE, ROWS), F8),
            vmem((WIDE, WIDE), F8),
            vmem((10, 1, 128), F32),
            vmem((10, 1, 128), F32),
            vmem((8, 2, 10, 1, 128), F32),
            vmem((8, 2, 10, 1, 128), F32),
            vmem((11, 128), F32),
            vmem((8, 11, 128), F32),
            vmem((1, 80), I32),
            vmem((1, 128), I32),
            dma,
            dma,
            dma((11,)),
            dma((3,)),
            dma((9,)),
            dma((8, 2)),
            dma((8, 2)),
            dma((64,)),
            dma((8,)),
        ],
        compiler_params=pltpu.CompilerParams(
            collective_id=0, has_side_effects=True, vmem_limit_bytes=56551552
        ),
    )(adjacency.T, relabel[None, :])
    return out[0], ratio[0, 0]


def solution(mesh):
    placed = (P("row", "col"), P(("row", "col")))
    return jax.shard_map(
        body, mesh=mesh, in_specs=placed, out_specs=(P(("row", "col")), P()), check_vma=False
    )
```

```python
import jax
import jax.numpy as jnp
from jax import lax
from jax.experimental import pallas as pl
from jax.experimental.pallas import tpu as pltpu
from jax.sharding import PartitionSpec as P

SENDS_A = (
    257605490, 171736168, 196289112, 247346300, 180321384, 187856101, 146221640, 163478224,
    180190828, 266059126, 239023736, 187834460, 196833529, 171867756, 154369748, 137766988,
    179511888, 263991412, 240696694, 196507744, 162998848, 146570968, 230520928, 170948321,
    255668848, 171057236, 188185188, 249151346, 137460444, 154544196, 179991281, 222067300,
    146504808, 155089645, 179511896, 196506816, 257603426, 137919592, 162998856, 213791852,
    163020529, 138051180, 188444868, 171057244, 146374252, 266057062, 205469288, 154544204,
    196289104, 179597512, 263813216, 138377445, 146221632, 230436964, 240694630, 162691168,
    171537612, 187834452, 146111733, 255359588, 222114400, 137766980, 154368612, 249149282,
)
SENDS_B = (
    1286998, 0, 0, 0, 0, 0, 0, 0,
    0, 1220946, 0, 0, 0, 0, 0, 0,
    0, 0, 1287006, 0, 0, 0, 0, 0,
    0, 0, 0, 1220954, 0, 0, 0, 0,
    0, 0, 0, 0, 1551174, 0, 0, 0,
    0, 0, 0, 0, 0, 1485122, 0, 0,
    0, 0, 0, 0, 0, 0, 1551182, 0,
    0, 0, 0, 0, 0, 0, 0, 1485130,
)
KIND = (
    0, 7, 2, 7, 3, 4, 0, 1,
    7, 0, 7, 0, 4, 3, 1, 0,
    2, 7, 0, 7, 0, 1, 3, 6,
    7, 0, 7, 0, 1, 0, 6, 3,
    3, 4, 0, 1, 0, 7, 0, 7,
    4, 3, 1, 0, 7, 0, 7, 2,
    0, 1, 3, 6, 0, 7, 0, 7,
    1, 0, 6, 3, 7, 2, 7, 0,
)

F8 = jnp.float8_e4m3fn
I32 = jnp.int32
F32 = jnp.float32
WORDS, ROWS, WIDE = 40, 640, 1280


def look_up(table, d):
    return sum(jnp.where(d == i, I32(v), I32(0)) for i, v in enumerate(table) if v)


def halves(words, top):
    twice = jnp.concatenate([words, words], axis=0)
    return jnp.where(top, twice & 0xFFFF, lax.shift_right_logical(twice, 16))


def unpacked(words, top, bits):
    part = halves(words, top)
    part = jnp.concatenate([part, part], axis=0).astype(jnp.int16)
    one, none = jnp.bfloat16(1), jnp.bfloat16(0)
    rows = [jnp.where((part & b) != 0, one, none) for b in bits]
    return [jnp.concatenate(rows[2 * j : 2 * j + 2], axis=0).astype(F8) for j in range(4)]


def kernel(
    adj, rel, out, ratio_out,
    plain, own, inbox, w_rhs, w_lhs, part_row, part_col, red_row, red_col, mine, every, rel_here, want_ref,
    adj_sem, rel_sem, send, relay_sem, in_sem, row_sem, col_sem, all_send, all_sem,
):
    row, col = lax.axis_index("row"), lax.axis_index("col")
    R, C, h = row // 2, col, row % 2
    g = 1 - h
    diag, off = R == C, R != C
    fetch = pltpu.make_async_copy(adj, plain, adj_sem)
    fetch.start()
    fetch_rel = pltpu.make_async_copy(rel, rel_here, rel_sem)
    fetch_rel.start()

    barrier = pltpu.get_barrier_semaphore()

    def hello(r, c):
        pl.semaphore_signal(barrier, inc=1, device_id={"row": r, "col": c})

    for i in range(1, 8):
        hello(row, (C + i) % 8)
        hello(2 * ((R + i) % 8) + h, C)
    hello(2 * R + g, C)

    place = R * 8 + C
    kinds = look_up(KIND, place)
    kind = kinds // 4
    codes_a, codes_b = look_up(SENDS_A, place), look_up(SENDS_B, place)
    lhs_is_own = diag | (kind == 1)
    rhs_is_own = kind == 0

    p = lax.broadcasted_iota(I32, (8, 128), 1)
    column = 32 * (p % 4) + 16 * (p // 4 % 2) + p // 8
    fetch.wait()

    @pl.loop(0, 5)
    def _(i):
        at = pl.ds(pl.multiple_of(i * 8, 8), 8)
        for k in range(5):
            lanes = slice(k * 128, (k + 1) * 128)
            own[at, lanes] = jnp.take_along_axis(plain[at, lanes], column, axis=1)


    @pl.when(lhs_is_own)
    def _():
        inbox[7 + h] = own[...]

    @pl.when(rhs_is_own)
    def _():
        inbox[2] = own[...]

    pl.semaphore_wait(barrier, 15)

    def copy(src, dst, ssem, rsem, r, c):
        return pltpu.make_async_remote_copy(
            src_ref=src, dst_ref=dst, send_sem=ssem, recv_sem=rsem,
            device_id={"row": r, "col": c},
        )

    def offer(i):
        code = (codes_a if i < 4 else codes_b) // (128 ** (i % 4)) % 128
        slot, to, down = code % 4, code // 4 % 8, code // 32 % 2
        box = jnp.where(down == 1, 3 + 2 * slot + h, slot)
        r = jnp.where(down == 1, 2 * to + h, row)
        c = jnp.where(down == 1, col, to)
        return code >= 64, copy(own, inbox.at[box], send.at[i], in_sem.at[box], r, c)

    for i in range(7):
        there, c = offer(i)
        pl.when(there)(c.start)

    def relay(s):
        box = 3 + 2 * s + h
        return copy(inbox.at[box], inbox.at[box], relay_sem.at[s], in_sem.at[box], 2 * R + g, C)

    def arrived(box):
        copy(own, inbox.at[box], send.at[0], in_sem.at[box], row, col).wait_recv()

    def pass_on(s):
        @pl.when((s < 2) | jnp.logical_not(lhs_is_own))
        def _():
            arrived(3 + 2 * s + h)

        relay(s).start()

    last = jnp.where(diag, 1, 3)
    degree = jnp.sum(lax.population_count(own[...]), axis=0, keepdims=True).astype(F32)
    part_row[...] = jnp.zeros_like(part_row)
    part_col[...] = jnp.zeros_like(part_col)
    for k in range(5):
        part_row[5 + k, :, :] = degree[:, k * 128 : (k + 1) * 128]
    pass_on(2)

    top = lax.broadcasted_iota(I32, (8, 128), 0) < 4
    upper = lax.broadcasted_iota(I32, (16, 128), 0) < 8
    bits = [
        jnp.where(upper, I32(1 << k), I32(1 << (k + 1) if k < 14 else -32768)).astype(jnp.int16)
        for k in range(0, 16, 2)
    ]

    def unpack(box, i, put):
        for k in range(5):
            words = inbox[box, pl.ds(pl.multiple_of(i * 8, 8), 8), k * 128 : (k + 1) * 128]
            for q in range(2):
                for j, piece in enumerate(unpacked(words[4 * q : 4 * q + 4], top, bits)):
                    put(q * 128 + j * 32, k * 128, piece)

    def product(lo, hi):
        for k in range(2):
            for i in range(lo, hi):
                def put(r, c, piece):
                    w_lhs[i * 256 + r : i * 256 + r + 32, k * ROWS + c : k * ROWS + c + 128] = piece
                unpack(3 + 2 * s_now[0] + k, i, put)
        at = slice(lo * 256, hi * 256)
        paths = jnp.dot(w_lhs[at, :], w_rhs[...], preferred_element_type=F32)
        closed = jnp.zeros((8, ROWS), F32)
        for n in range(2 * (hi - lo)):
            words = own[(2 * lo + n) * 4 : (2 * lo + n) * 4 + 4, :]
            part = halves(words, wide_top)
            sums = []
            for k in range(16):
                r = n * 128 + k * 8
                val = jnp.where((part & (1 << k)) != 0, paths[r : r + 8, :], 0.0)
                closed = closed + val
                sums.append(sum(val[:, j * 128 : (j + 1) * 128] for j in range(5)))
            across = jnp.sum(jnp.concatenate(sums, axis=0).T, axis=0, keepdims=True)
            part_col[2 * lo + n, :, :] += across * (2.0 - t_now[0])
        closed = jnp.sum(closed, axis=0, keepdims=True) * (1.0 + t_now[0])
        for k in range(5):
            part_row[k, :, :] += closed[:, k * 128 : (k + 1) * 128]

    wide_top = lax.broadcasted_iota(I32, (8, ROWS), 0) < 4
    s_now, t_now = [None], [None]

    @pl.loop(0, last)
    def _(turn):
        s = (turn + 2) % 3

        @pl.when((s < 2) | jnp.logical_not(rhs_is_own))
        def _():
            arrived(s)

        for i in range(5):
            def put(r, c, piece):
                w_rhs[i * 256 + r : i * 256 + r + 32, c : c + 128] = piece
            unpack(s, i, put)

        @pl.when(turn + 1 < last)
        def _():
            pass_on(turn)

        arrived(3 + 2 * s + g)
        s_now[0] = s
        t_now[0] = jnp.where(
            s == 0, kinds % 2, jnp.where(s == 1, kinds // 2 % 2, kind)
        ).astype(F32)
        product(0, 3)

        product(3, 5)

    give_row = [
        copy(part_row, red_row.at[C, h], send.at[7 + k], row_sem.at[C, h], 2 * R + k, R)
        for k in range(2)
    ]
    give_col = [
        copy(part_col, red_col.at[R, h], send.at[9 + k], col_sem.at[R, h], 2 * C + k, C)
        for k in range(2)
    ]

    @pl.when(off)
    def _():
        for c in give_row + give_col:
            c.start()

    to_other = copy(part_row, red_row.at[C, h], send.at[7], row_sem.at[C, h], 2 * R + g, C)
    pl.when(diag)(to_other.start)

    def tell(r, c):
        return copy(mine, every.at[R], all_send.at[r // 2 * 8 + c], all_sem.at[R], r, c)

    def for_all(act):
        where = [(x, y, z) for x in range(4) for y in range(4) for z in range(4)]
        where.sort(key=lambda v: sum(min(a, 4 - a) for a in v))
        for x, y, z in where:
            r, c = y * 4 + x % 2 * 2 + h, x // 2 * 4 + z

            @pl.when((r != row) | (c != col))
            def _():
                act(tell(r, c))

    @pl.when(diag)
    def _():
        copy(part_row, red_row.at[C, g], send.at[0], row_sem.at[C, g], row, col).wait_recv()
        red_row[C, h] = part_row[...]
        flat = jnp.zeros((10, 1, 128), F32)

        def add(i, carry):
            closed, degree, across = carry
            o = (R + i) % 8
            for k in range(2):
                copy(
                    part_row, red_row.at[o, k], send.at[0], row_sem.at[o, k], row, col
                ).wait_recv()
                copy(
                    part_col, red_col.at[o, k], send.at[0], col_sem.at[o, k], row, col
                ).wait_recv()
                across = across + red_col[o, k]
            sums = [red_row[o, k] for k in range(2)]
            closed = closed + jnp.concatenate([v[:5] for v in sums], axis=0)
            degree = degree + jnp.concatenate([v[5:] for v in sums], axis=0)
            return closed, degree, across

        sums = [red_row[C, k] for k in range(2)]
        closed = jnp.concatenate([v[:5] for v in sums], axis=0)
        degree = jnp.concatenate([v[5:] for v in sums], axis=0)
        closed, degree, across = lax.fori_loop(1, 8, add, (closed, degree, flat))
        total, deg = (closed + across)[:, 0, :], degree[:, 0, :]
        wedges = jnp.maximum(deg * (deg - 1.0), 1.0)
        mine[0:10, :] = total / wedges
        low = lax.broadcasted_iota(I32, (1, 128), 1) < 64
        both = []
        for v in (total, wedges):
            v = jnp.sum(v, axis=0, keepdims=True)
            both.append(v + pltpu.roll(v, 64, 1))
        mine[10:11, :] = jnp.where(low, both[0], both[1])
        every[C] = mine[...]
        for_all(lambda c: c.start())

    want_ref[...] = jnp.zeros_like(want_ref)
    fetch_rel.wait()
    want_ref[:, 0:80] = rel_here[...]
    want = jnp.broadcast_to(want_ref[...], (11, 128))
    block, rest = want // WIDE, want % WIDE
    line, lane = rest // 128, rest % 128
    lane = 8 * (lane % 16) + 4 * (lane // 16 % 2) + lane // 32
    here = lax.broadcasted_iota(I32, (11, 128), 0) == line

    for i in range(7):
        there, c = offer(i)
        pl.when(there)(c.wait_send)

    @pl.loop(0, last)
    def _(turn):
        relay((turn + 2) % 3).wait_send()

    @pl.when(off)
    def _():
        for c in give_row + give_col:
            c.wait_send()

    pl.when(diag)(to_other.wait_send)

    @pl.when(diag)
    def _():
        for_all(lambda c: c.wait_send())

    found = jnp.zeros((11, 128), F32)
    sums = jnp.zeros((1, 128), F32)
    for b in range(8):
        @pl.when(off | (R != b))
        def _():
            copy(mine, every.at[b], all_send.at[0], all_sem.at[b], row, col).wait_recv()

        tile = every[b]
        sums = sums + tile[10:11, :]
        got = jnp.take_along_axis(tile, lane, axis=1)
        found = found + jnp.where(here & (block == b), got, 0.0)
    low = lax.broadcasted_iota(I32, (1, 128), 1) < 64
    top = jnp.sum(jnp.where(low, sums, 0.0), axis=1, keepdims=True)
    bottom = jnp.sum(jnp.where(low, 0.0, sums), axis=1, keepdims=True)
    ratio_out[...] = top / bottom
    out[...] = jnp.sum(found, axis=0, keepdims=True)[:, 0:80]


def body(adjacency, relabel):
    dma = pltpu.SemaphoreType.DMA
    vmem = pltpu.VMEM
    out, ratio = pl.pallas_call(
        kernel,
        out_shape=(jax.ShapeDtypeStruct((1, 80), F32), jax.ShapeDtypeStruct((1, 1), F32)),
        in_specs=[pl.BlockSpec(memory_space=pl.ANY)] * 2,
        out_specs=[pl.BlockSpec(memory_space=vmem)] * 2,
        scratch_shapes=[
            vmem((WORDS, ROWS), I32),
            vmem((WORDS, ROWS), I32),
            vmem((9, WORDS, ROWS), I32),
            vmem((WIDE, ROWS), F8),
            vmem((WIDE, WIDE), F8),
            vmem((10, 1, 128), F32),
            vmem((10, 1, 128), F32),
            vmem((8, 2, 10, 1, 128), F32),
            vmem((8, 2, 10, 1, 128), F32),
            vmem((11, 128), F32),
            vmem((8, 11, 128), F32),
            vmem((1, 80), I32),
            vmem((1, 128), I32),
            dma,
            dma,
            dma((11,)),
            dma((3,)),
            dma((9,)),
            dma((8, 2)),
            dma((8, 2)),
            dma((64,)),
            dma((8,)),
        ],
        compiler_params=pltpu.CompilerParams(
            collective_id=0, has_side_effects=True, vmem_limit_bytes=56551552
        ),
    )(adjacency.T, relabel[None, :])
    return out[0], ratio[0, 0]


def solution(mesh):
    placed = (P("row", "col"), P(("row", "col")))
    return jax.shard_map(
        body, mesh=mesh, in_specs=placed, out_specs=(P(("row", "col")), P()), check_vma=False
    )
```

```python
import jax
import jax.numpy as jnp
from jax import lax
from jax.experimental import pallas as pl
from jax.experimental.pallas import tpu as pltpu
from jax.sharding import PartitionSpec as P

SENDS_A = (
    257605490, 171736168, 196289112, 247346300, 180321384, 187856101, 146221640, 163478224,
    180190828, 266059126, 239023736, 187834460, 196833529, 171867756, 154369748, 137766988,
    179511888, 263991412, 240696694, 196507744, 162998848, 146570968, 230520928, 170948321,
    255668848, 171057236, 188185188, 249151346, 137460444, 154544196, 179991281, 222067300,
    146504808, 155089645, 179511896, 196506816, 257603426, 137919592, 162998856, 213791852,
    163020529, 138051180, 188444868, 171057244, 146374252, 266057062, 205469288, 154544204,
    196289104, 179597512, 263813216, 138377445, 146221632, 230436964, 240694630, 162691168,
    171537612, 187834452, 146111733, 255359588, 222114400, 137766980, 154368612, 249149282,
)
SENDS_B = (
    1286998, 0, 0, 0, 0, 0, 0, 0,
    0, 1220946, 0, 0, 0, 0, 0, 0,
    0, 0, 1287006, 0, 0, 0, 0, 0,
    0, 0, 0, 1220954, 0, 0, 0, 0,
    0, 0, 0, 0, 1551174, 0, 0, 0,
    0, 0, 0, 0, 0, 1485122, 0, 0,
    0, 0, 0, 0, 0, 0, 1551182, 0,
    0, 0, 0, 0, 0, 0, 0, 1485130,
)
KIND = (
    0, 7, 2, 7, 3, 4, 0, 1,
    7, 0, 7, 0, 4, 3, 1, 0,
    2, 7, 0, 7, 0, 1, 3, 6,
    7, 0, 7, 0, 1, 0, 6, 3,
    3, 4, 0, 1, 0, 7, 0, 7,
    4, 3, 1, 0, 7, 0, 7, 2,
    0, 1, 3, 6, 0, 7, 0, 7,
    1, 0, 6, 3, 7, 2, 7, 0,
)

F8 = jnp.float8_e4m3fn
I32 = jnp.int32
F32 = jnp.float32
WORDS, ROWS, WIDE = 40, 640, 1280


def look_up(table, d):
    return sum(jnp.where(d == i, I32(v), I32(0)) for i, v in enumerate(table) if v)


def halves(words, top):
    twice = jnp.concatenate([words, words], axis=0)
    return jnp.where(top, twice & 0xFFFF, lax.shift_right_logical(twice, 16))


def unpacked(words, top, bits):
    part = halves(words, top)
    part = jnp.concatenate([part, part], axis=0).astype(jnp.int16)
    one, none = jnp.bfloat16(1), jnp.bfloat16(0)
    rows = [jnp.where((part & b) != 0, one, none) for b in bits]
    return [jnp.concatenate(rows[2 * j : 2 * j + 2], axis=0).astype(F8) for j in range(4)]


def kernel(
    adj, rel, out, ratio_out,
    plain, own, inbox, w_rhs, w_lhs, part_row, part_col, red_row, red_col, mine, every, rel_here, want_ref,
    adj_sem, rel_sem, send, relay_sem, in_sem, row_sem, col_sem, all_send, all_sem,
):
    row, col = lax.axis_index("row"), lax.axis_index("col")
    R, C, h = row // 2, col, row % 2
    g = 1 - h
    diag, off = R == C, R != C
    fetch = pltpu.make_async_copy(adj, plain, adj_sem)
    fetch.start()
    fetch_rel = pltpu.make_async_copy(rel, rel_here, rel_sem)
    fetch_rel.start()

    barrier = pltpu.get_barrier_semaphore()

    def hello(r, c):
        pl.semaphore_signal(barrier, inc=1, device_id={"row": r, "col": c})

    for i in range(1, 8):
        hello(row, (C + i) % 8)
        hello(2 * ((R + i) % 8) + h, C)
    hello(2 * R + g, C)

    place = R * 8 + C
    kinds = look_up(KIND, place)
    kind = kinds // 4
    codes_a, codes_b = look_up(SENDS_A, place), look_up(SENDS_B, place)
    lhs_is_own = diag | (kind == 1)
    rhs_is_own = kind == 0

    p = lax.broadcasted_iota(I32, (8, 128), 1)
    column = 32 * (p % 4) + 16 * (p // 4 % 2) + p // 8
    fetch.wait()

    @pl.loop(0, 5)
    def _(i):
        at = pl.ds(pl.multiple_of(i * 8, 8), 8)
        for k in range(5):
            lanes = slice(k * 128, (k + 1) * 128)
            own[at, lanes] = jnp.take_along_axis(plain[at, lanes], column, axis=1)


    @pl.when(lhs_is_own)
    def _():
        inbox[7 + h] = own[...]

    @pl.when(rhs_is_own)
    def _():
        inbox[2] = own[...]

    pl.semaphore_wait(barrier, 15)

    def copy(src, dst, ssem, rsem, r, c):
        return pltpu.make_async_remote_copy(
            src_ref=src, dst_ref=dst, send_sem=ssem, recv_sem=rsem,
            device_id={"row": r, "col": c},
        )

    def offer(i):
        code = (codes_a if i < 4 else codes_b) // (128 ** (i % 4)) % 128
        slot, to, down = code % 4, code // 4 % 8, code // 32 % 2
        box = jnp.where(down == 1, 3 + 2 * slot + h, slot)
        r = jnp.where(down == 1, 2 * to + h, row)
        c = jnp.where(down == 1, col, to)
        return code >= 64, copy(own, inbox.at[box], send.at[i], in_sem.at[box], r, c)

    for i in range(7):
        there, c = offer(i)
        pl.when(there)(c.start)

    def relay(s):
        box = 3 + 2 * s + h
        return copy(inbox.at[box], inbox.at[box], relay_sem.at[s], in_sem.at[box], 2 * R + g, C)

    def arrived(box):
        copy(own, inbox.at[box], send.at[0], in_sem.at[box], row, col).wait_recv()

    def pass_on(s):
        @pl.when((s < 2) | jnp.logical_not(lhs_is_own))
        def _():
            arrived(3 + 2 * s + h)

        relay(s).start()

    last = jnp.where(diag, 1, 3)
    degree = jnp.sum(lax.population_count(own[...]), axis=0, keepdims=True).astype(F32)
    part_row[...] = jnp.zeros_like(part_row)
    part_col[...] = jnp.zeros_like(part_col)
    for k in range(5):
        part_row[5 + k, :, :] = degree[:, k * 128 : (k + 1) * 128]
    pass_on(2)

    top = lax.broadcasted_iota(I32, (8, 128), 0) < 4
    upper = lax.broadcasted_iota(I32, (16, 128), 0) < 8
    bits = [
        jnp.where(upper, I32(1 << k), I32(1 << (k + 1) if k < 14 else -32768)).astype(jnp.int16)
        for k in range(0, 16, 2)
    ]

    def unpack(box, i, put):
        for k in range(5):
            words = inbox[box, pl.ds(pl.multiple_of(i * 8, 8), 8), k * 128 : (k + 1) * 128]
            for q in range(2):
                for j, piece in enumerate(unpacked(words[4 * q : 4 * q + 4], top, bits)):
                    put(q * 128 + j * 32, k * 128, piece)

    def product(lo, hi):
        for k in range(2):
            for i in range(lo, hi):
                def put(r, c, piece):
                    w_lhs[i * 256 + r : i * 256 + r + 32, k * ROWS + c : k * ROWS + c + 128] = piece
                unpack(3 + 2 * s_now[0] + k, i, put)
        at = slice(lo * 256, hi * 256)
        paths = jnp.dot(w_lhs[at, :], w_rhs[...], preferred_element_type=F32)
        closed = jnp.zeros((8, ROWS), F32)
        for n in range(2 * (hi - lo)):
            words = own[(2 * lo + n) * 4 : (2 * lo + n) * 4 + 4, :]
            part = halves(words, wide_top)
            sums = []
            for k in range(16):
                r = n * 128 + k * 8
                val = jnp.where((part & (1 << k)) != 0, paths[r : r + 8, :], 0.0)
                closed = closed + val
                sums.append(sum(val[:, j * 128 : (j + 1) * 128] for j in range(5)))
            across = jnp.sum(jnp.concatenate(sums, axis=0).T, axis=0, keepdims=True)
            part_col[2 * lo + n, :, :] += across * (2.0 - t_now[0])
        closed = jnp.sum(closed, axis=0, keepdims=True) * (1.0 + t_now[0])
        for k in range(5):
            part_row[k, :, :] += closed[:, k * 128 : (k + 1) * 128]

    wide_top = lax.broadcasted_iota(I32, (8, ROWS), 0) < 4
    s_now, t_now = [None], [None]

    @pl.loop(0, last)
    def _(turn):
        s = (turn + 2) % 3

        @pl.when((s < 2) | jnp.logical_not(rhs_is_own))
        def _():
            arrived(s)

        @pl.loop(0, 5)
        def _(i):
            def put(r, c, piece):
                w_rhs[pl.ds(pl.multiple_of(i * 256 + r, 32), 32), c : c + 128] = piece
            unpack(s, i, put)

        arrived(3 + 2 * s + g)

        @pl.when(turn + 1 < last)
        def _():
            pass_on(turn)

        s_now[0] = s
        t_now[0] = jnp.where(
            s == 0, kinds % 2, jnp.where(s == 1, kinds // 2 % 2, kind)
        ).astype(F32)
        product(0, 3)

        product(3, 5)

    give_row = [
        copy(part_row, red_row.at[C, h], send.at[7 + k], row_sem.at[C, h], 2 * R + k, R)
        for k in range(2)
    ]
    give_col = [
        copy(part_col, red_col.at[R, h], send.at[9 + k], col_sem.at[R, h], 2 * C + k, C)
        for k in range(2)
    ]

    @pl.when(off)
    def _():
        for c in give_row + give_col:
            c.start()

    to_other = copy(part_row, red_row.at[C, h], send.at[7], row_sem.at[C, h], 2 * R + g, C)
    pl.when(diag)(to_other.start)

    def tell(r, c):
        return copy(mine, every.at[R], all_send.at[r // 2 * 8 + c], all_sem.at[R], r, c)

    def for_all(act):
        where = [(x, y, z) for x in range(4) for y in range(4) for z in range(4)]
        where.sort(key=lambda v: min(v[0], 4 - v[0]) + min(v[1], 4 - v[1]) + v[2])
        for x, y, z in where:
            r, c = y * 4 + x % 2 * 2 + h, x // 2 * 4 + z

            @pl.when((r != row) | (c != col))
            def _():
                act(tell(r, c))

    @pl.when(diag)
    def _():
        copy(part_row, red_row.at[C, g], send.at[0], row_sem.at[C, g], row, col).wait_recv()
        red_row[C, h] = part_row[...]
        flat = jnp.zeros((10, 1, 128), F32)

        def add(i, carry):
            closed, degree, across = carry
            o = (R + i) % 8
            for k in range(2):
                copy(
                    part_row, red_row.at[o, k], send.at[0], row_sem.at[o, k], row, col
                ).wait_recv()
                copy(
                    part_col, red_col.at[o, k], send.at[0], col_sem.at[o, k], row, col
                ).wait_recv()
                across = across + red_col[o, k]
            sums = [red_row[o, k] for k in range(2)]
            closed = closed + jnp.concatenate([v[:5] for v in sums], axis=0)
            degree = degree + jnp.concatenate([v[5:] for v in sums], axis=0)
            return closed, degree, across

        sums = [red_row[C, k] for k in range(2)]
        closed = jnp.concatenate([v[:5] for v in sums], axis=0)
        degree = jnp.concatenate([v[5:] for v in sums], axis=0)
        closed, degree, across = lax.fori_loop(1, 8, add, (closed, degree, flat))
        total, deg = (closed + across)[:, 0, :], degree[:, 0, :]
        wedges = jnp.maximum(deg * (deg - 1.0), 1.0)
        mine[0:10, :] = total / wedges
        low = lax.broadcasted_iota(I32, (1, 128), 1) < 64
        both = []
        for v in (total, wedges):
            v = jnp.sum(v, axis=0, keepdims=True)
            both.append(v + pltpu.roll(v, 64, 1))
        mine[10:11, :] = jnp.where(low, both[0], both[1])
        every[C] = mine[...]
        for_all(lambda c: c.start())

    want_ref[...] = jnp.zeros_like(want_ref)
    fetch_rel.wait()
    want_ref[:, 0:80] = rel_here[...]
    want = jnp.broadcast_to(want_ref[...], (11, 128))
    block, rest = want // WIDE, want % WIDE
    line, lane = rest // 128, rest % 128
    lane = 8 * (lane % 16) + 4 * (lane // 16 % 2) + lane // 32
    here = lax.broadcasted_iota(I32, (11, 128), 0) == line

    for i in range(7):
        there, c = offer(i)
        pl.when(there)(c.wait_send)

    @pl.loop(0, last)
    def _(turn):
        relay((turn + 2) % 3).wait_send()

    @pl.when(off)
    def _():
        for c in give_row + give_col:
            c.wait_send()

    pl.when(diag)(to_other.wait_send)

    @pl.when(diag)
    def _():
        for_all(lambda c: c.wait_send())

    found = jnp.zeros((11, 128), F32)
    sums = jnp.zeros((1, 128), F32)
    for b in range(8):
        @pl.when(off | (R != b))
        def _():
            copy(mine, every.at[b], all_send.at[0], all_sem.at[b], row, col).wait_recv()

        tile = every[b]
        sums = sums + tile[10:11, :]
        got = jnp.take_along_axis(tile, lane, axis=1)
        found = found + jnp.where(here & (block == b), got, 0.0)
    low = lax.broadcasted_iota(I32, (1, 128), 1) < 64
    top = jnp.sum(jnp.where(low, sums, 0.0), axis=1, keepdims=True)
    bottom = jnp.sum(jnp.where(low, 0.0, sums), axis=1, keepdims=True)
    ratio_out[...] = top / bottom
    out[...] = jnp.sum(found, axis=0, keepdims=True)[:, 0:80]


def body(adjacency, relabel):
    dma = pltpu.SemaphoreType.DMA
    vmem = pltpu.VMEM
    out, ratio = pl.pallas_call(
        kernel,
        out_shape=(jax.ShapeDtypeStruct((1, 80), F32), jax.ShapeDtypeStruct((1, 1), F32)),
        in_specs=[pl.BlockSpec(memory_space=pl.ANY)] * 2,
        out_specs=[pl.BlockSpec(memory_space=vmem)] * 2,
        scratch_shapes=[
            vmem((WORDS, ROWS), I32),
            vmem((WORDS, ROWS), I32),
            vmem((9, WORDS, ROWS), I32),
            vmem((WIDE, ROWS), F8),
            vmem((WIDE, WIDE), F8),
            vmem((10, 1, 128), F32),
            vmem((10, 1, 128), F32),
            vmem((8, 2, 10, 1, 128), F32),
            vmem((8, 2, 10, 1, 128), F32),
            vmem((11, 128), F32),
            vmem((8, 11, 128), F32),
            vmem((1, 80), I32),
            vmem((1, 128), I32),
            dma,
            dma,
            dma((11,)),
            dma((3,)),
            dma((9,)),
            dma((8, 2)),
            dma((8, 2)),
            dma((64,)),
            dma((8,)),
        ],
        compiler_params=pltpu.CompilerParams(
            collective_id=0, has_side_effects=True, vmem_limit_bytes=56551552
        ),
    )(adjacency.T, relabel[None, :])
    return out[0], ratio[0, 0]


def solution(mesh):
    placed = (P("row", "col"), P(("row", "col")))
    return jax.shard_map(
        body, mesh=mesh, in_specs=placed, out_specs=(P(("row", "col")), P()), check_vma=False
    )
```
